256 devices in a mesh: samp: 32 (over y, z_hi, x), tile: 8 (over z_lo, core).
Axes of the slice: x: 4, y: 4, z: 8 (z_hi: 2, z_lo: 4; z = z_hi * 4 + z_lo), core: 2. Of those that a mesh axis runs over, the one named last changes fastest.
Arguments:
- traits: bfloat16 [32768, 1024], P('samp'), may hold values from -300 to 300
- covariates: bfloat16 [32768, 32], P('samp'), may hold values from -6 to 6
- genotypes: int32 [32768, 2048], P('samp', 'tile'), may hold values from 0 to 2
- shuffles: int32 [6, 32768], P(None, 'samp'), may hold values from 0 to 32767, as said below
Outputs:
- observed: float32 [1024, 2048], P('samp', 'tile')
- perm_max: float32 [6, 1024], P(None, 'samp')
The draws below stay inside these ranges and needn't reach their ends.
Inputs may be any that keep to these rules, and one draw needn't show every extreme that they name: Row p of shuffles maps each aligned block of 1024 samples one to one onto the same block's samples.
All inputs are finite; a program needn't handle non-finite values.
Results may differ from the reference program's by a relative error of at most 0.0045.
Values sent between devices are 32-bit elements; how exact they have to be, the bound alone decides.
No kernel may reach another device: no remote copies, remote signals or barrier semaphores. Data moves between devices by JAX's collectives and lax.ppermute only.
A program may use at most 64 MiB of HBM per device.

```python
import math
import jax
import jax.numpy as jnp
from jax import lax

SAMP_DEV = 1024
E = 1024
C = 32
PERMS = 6
SAMPLES = 32768
VARIANTS = 2048


def covariate_base(key):
    values = jax.random.normal(jax.random.fold_in(key, 11), (SAMPLES, C), jnp.float32)
    return jnp.clip(values, -6.0, 6.0)


def draw_covariates(key, part):
    return covariate_base(key).astype(jnp.bfloat16)


def draw_traits(key, part):
    base = covariate_base(key)
    key_load, key_mean, key_noise, key_cols = jax.random.split(jax.random.fold_in(key, 23), 4)
    loading = jax.random.normal(key_load, (C, E), jnp.float32) / math.sqrt(C)
    means = 2.0 * jnp.clip(jax.random.normal(key_mean, (E,), jnp.float32), -4.0, 4.0)
    col_scale = jnp.exp(jax.random.uniform(key_cols, (E,), jnp.float32, 0.0, math.log(10.0)))
    position = jnp.arange(SAMPLES, dtype=jnp.float32) / SAMPLES
    noise = jnp.clip(jax.random.normal(key_noise, (SAMPLES, E), jnp.float32), -5.0, 5.0)
    row_scale = 1.0 + 2.0 * position
    fitted = jnp.dot(base, loading, precision=lax.Precision.HIGHEST)
    values = (means[None, :] + fitted + noise) * row_scale[:, None] * col_scale[None, :]
    return jnp.clip(values, -300.0, 300.0).astype(jnp.bfloat16)


def draw_genotypes(key, part):
    key_freq, key_first, key_second = jax.random.split(jax.random.fold_in(key, 37), 3)
    freq = jax.random.randint(key_freq, (1, VARIANTS), 5, 96)
    first = (jax.random.randint(key_first, (SAMPLES, VARIANTS), 0, 100) < freq).astype(jnp.int32)
    second = (jax.random.randint(key_second, (SAMPLES, VARIANTS), 0, 100) < freq).astype(jnp.int32)
    return first + second


def draw_shuffles(key, part):
    blocks = SAMPLES // SAMP_DEV
    keys = jax.random.split(jax.random.fold_in(key, 41), PERMS * blocks)
    orders = jax.vmap(lambda one_key: jax.random.permutation(one_key, SAMP_DEV))(keys).astype(jnp.int32)
    offsets = jnp.arange(blocks, dtype=jnp.int32) * SAMP_DEV
    orders = orders.reshape(PERMS, blocks, SAMP_DEV) + offsets[None, :, None]
    return orders.reshape(PERMS, SAMPLES).astype(jnp.int32)


def setup_inputs(seed: int = 0) -> dict:
    key_of = jax.random.split(jax.random.key(seed), 5)
    return {
        "traits": draw_traits(jax.random.fold_in(key_of[4], 71), 0),
        "covariates": draw_covariates(jax.random.fold_in(key_of[4], 71), 0),
        "genotypes": draw_genotypes(jax.random.fold_in(key_of[4], 71), 0),
        "shuffles": draw_shuffles(jax.random.fold_in(key_of[4], 71), 0),
    }


epsilon = 1e-05

def cholesky_solve(factor, rhs):
    first = lax.linalg.triangular_solve(factor, rhs, left_side=True, lower=True)
    return lax.linalg.triangular_solve(factor, first, left_side=True, lower=True, transpose_a=True)

def reference(traits, covariates, genotypes, shuffles):
    ones = jnp.ones((covariates.shape[0], 1), jnp.bfloat16)
    design = jnp.concatenate([ones, covariates], axis=1)
    dosage = genotypes.astype(jnp.bfloat16)
    gram = jnp.dot(design.T.astype(jnp.float32), design.astype(jnp.float32), preferred_element_type=jnp.float32)
    xty = jnp.dot(design.T.astype(jnp.float32), traits.astype(jnp.float32), preferred_element_type=jnp.float32)
    xtg = jnp.dot(design.T.astype(jnp.float32), dosage.astype(jnp.float32), preferred_element_type=jnp.float32)
    factor = jnp.linalg.cholesky(gram)
    coef_traits = cholesky_solve(factor, xty).astype(jnp.bfloat16)
    coef_geno = cholesky_solve(factor, xtg).astype(jnp.bfloat16)
    resid_traits = traits.astype(jnp.float32) - jnp.dot(design.astype(jnp.float32), coef_traits.astype(jnp.float32), preferred_element_type=jnp.float32)
    resid_geno = dosage.astype(jnp.float32) - jnp.dot(design.astype(jnp.float32), coef_geno.astype(jnp.float32), preferred_element_type=jnp.float32)
    mean_traits = lax.optimization_barrier(jnp.sum(resid_traits * resid_traits, axis=0)) / SAMPLES
    mean_geno = lax.optimization_barrier(jnp.sum(resid_geno * resid_geno, axis=0)) / SAMPLES
    rt_rows = resid_traits.astype(jnp.bfloat16)
    rg_rows = resid_geno.astype(jnp.bfloat16)
    scale_traits = lax.rsqrt(mean_traits + epsilon)
    scale_geno = lax.rsqrt(mean_geno + epsilon)
    factor_z = math.sqrt(SAMPLES - C - 2) / SAMPLES

    def scores_of(trait_rows):
        cross = jnp.dot(trait_rows.T.astype(jnp.float32), rg_rows.astype(jnp.float32), preferred_element_type=jnp.float32)
        return cross * scale_traits[:, None] * scale_geno[None, :] * factor_z
    observed = scores_of(rt_rows)

    def one_perm(order):
        shuffled = jnp.take(rt_rows, order.astype(jnp.int32), axis=0)
        return lax.optimization_barrier(jnp.max(jnp.abs(scores_of(shuffled)), axis=1))
    perm_max = lax.map(one_perm, shuffles)
    return (observed, perm_max)
```

```python
import math

import jax
import jax.numpy as jnp
from jax import lax
from jax.experimental import pallas as pl
from jax.experimental.pallas import tpu as pltpu
from jax.sharding import Mesh, PartitionSpec as P

C = 32
EPSILON = 1e-05

ROWS = 1024
E = 1024
V = 256
PERMS = 6
HALF = E // 2
COLS = V + HALF + 128
CHUNK = (PERMS + 1) * V // 2
F32 = jnp.float32
BF16 = jnp.bfloat16


def dot(a, b):
    return jnp.dot(a, b, preferred_element_type=F32)


def call(kernel, outs, *args, grid_spec=None, flops=0, name=None):
    shapes = [jax.ShapeDtypeStruct(s, d) for s, d in outs]
    single = len(shapes) == 1
    extra = {} if grid_spec is None else {"grid_spec": grid_spec}
    nbytes = sum(math.prod(s) * jnp.dtype(d).itemsize for s, d in outs)
    return pl.pallas_call(
        kernel,
        out_shape=shapes[0] if single else shapes,
        name=name,
        cost_estimate=pl.CostEstimate(flops=flops, bytes_accessed=nbytes, transcendentals=0),
        **extra,
    )(*args)


def shifts(axis, k):
    n = lax.axis_size(axis)
    return [(i, (i + k) % n) for i in range(n)]


def shift(value, axis, k):
    return lax.ppermute(value, axis, shifts(axis, k))


def total_over(value, axis):
    if lax.axis_size(axis) == 2:
        return value + shift(value, axis, 1)
    one, two, three = (shift(value, axis, k) for k in (1, 2, 3))
    return (value + two) + (one + three)


def front_kernel(core_ref, traits_ref, cov_ref, geno_ref, pay_ref, xt_ref, dx_ref):
    del core_ref
    cov = cov_ref[...].astype(F32)
    lane = lax.broadcasted_iota(jnp.int32, (ROWS, 128 - C), 1)
    tail = jnp.where(lane == 0, 1.0, 0.0).astype(F32)
    design = jnp.concatenate([cov, tail], axis=1)
    dosage = geno_ref[...].astype(F32).astype(BF16)
    design_b = design.astype(BF16)
    dx_ref[:, :V] = dosage
    dx_ref[:, V:] = design_b
    xt = jnp.transpose(design)[:48].astype(BF16)
    xt_ref[...] = xt
    pay_ref[:, :V] = dot(xt, dosage)[:40]
    pay_ref[:, V : V + HALF] = dot(xt, traits_ref[...])[:40]
    pay_ref[:, V + HALF :] = dot(xt, design_b)[:40]


def turn_kernel(traits_ref, out_ref):
    out_ref[...] = jnp.transpose(traits_ref[...])


def perm_kernel(base_ref, order_ref, dx_ref, out_ref):
    order = order_ref[0] - base_ref[0]
    for at in range(0, ROWS, 256):
        row = lax.broadcasted_iota(jnp.int32, (256, ROWS), 0) + at
        pick = jnp.where(row == order, 1.0, 0.0).astype(BF16)
        out_ref[0, at : at + 256, :] = dot(pick, dx_ref[...]).astype(BF16)


def solve_kernel(own_ref, far_ref, out_ref):
    m = own_ref[...] + far_ref[...]
    row_id = lax.broadcasted_iota(jnp.int32, (40, COLS), 0)
    for k in range(C + 1):
        at = V + HALF + k
        col = m[:, at : at + 1]
        row = m[k : k + 1, :] / m[k : k + 1, at : at + 1]
        m = jnp.where(row_id == k, row, m - col * row)
    out_ref[...] = m[:, : V + HALF]


def resid_kernel(core_ref, own_ref, far_ref, yt_ref, xt_ref, dx_ref, dxp_ref, rt_ref, g1_ref, g2_ref, ss_ref):
    core = core_ref[0]
    xt = xt_ref[...]
    zeros = jnp.zeros((8, E), F32)
    mine = own_ref[:, V:]
    other = far_ref[...]
    first = jnp.where(core == 0, mine, other)
    second = jnp.where(core == 0, other, mine)
    coef = jnp.concatenate([jnp.concatenate([first, second], axis=1), zeros], axis=0)
    coef_t = jnp.transpose(coef).astype(BF16)
    ss_parts = []
    for at in range(0, E, 128):
        res = yt_ref[at : at + 128, :].astype(F32) - dot(coef_t[at : at + 128], xt)
        rt_ref[at : at + 128, :] = res.astype(BF16)
        sq = res * res
        lanes = sq[:, :128]
        for b in range(128, ROWS, 128):
            lanes = lanes + sq[:, b : b + 128]
        ss_parts.append(jnp.sum(jnp.transpose(lanes), axis=0, keepdims=True))
    gamma = jnp.concatenate([own_ref[:, :V], jnp.zeros((88, V), F32)], axis=0).astype(BF16)
    res_g = dx_ref[:, :V].astype(F32) - dot(dx_ref[:, V:], gamma)
    g1_ref[:, :V] = res_g.astype(BF16)
    ss_v = jnp.sum(res_g * res_g, axis=0, keepdims=True)
    for p in range(PERMS):
        g = (dxp_ref[p, :, :V].astype(F32) - dot(dxp_ref[p, :, V:], gamma)).astype(BF16)
        at = (p + 1) * V
        if at + V <= CHUNK:
            g1_ref[:, at : at + V] = g
        elif at >= CHUNK:
            g2_ref[:, at - CHUNK : at - CHUNK + V] = g
        else:
            g1_ref[:, at:] = g[:, : CHUNK - at]
            g2_ref[:, : at + V - CHUNK] = g[:, CHUNK - at :]
    ss_ref[...] = jnp.zeros((8, CHUNK), F32)
    ss_ref[0:1, :] = jnp.concatenate(ss_parts[:7], axis=1)
    ss_ref[1:2, :128] = ss_parts[7]
    ss_ref[1:2, 128 : 128 + V] = ss_v


def cross1_kernel(to_ref, rt_ref, g_ref, ss_ref, out_ref):
    del to_ref
    rows = rt_ref[...].reshape(256, ROWS)
    out_ref[:256, :] = dot(rows, g_ref[...])
    out_ref[256:, :] = ss_ref[...]


def cross2_kernel(to_ref, rt_ref, g_ref, out_ref):
    del to_ref
    out_ref[...] = dot(rt_ref[...], g_ref[...])


def mid1_kernel(at_ref, a, b, c, d, *outs):
    y = at_ref[0]
    ss = (a[256:, :] + c[256:, :]) + (b[256:, :] + d[256:, :])
    for k in range(4):
        at = pl.multiple_of(((y + k) % 4) * 64, 64)
        rows = pl.ds(at, 64)
        outs[k][:64, :] = (a[rows, :] + c[rows, :]) + (b[rows, :] + d[rows, :])
        outs[k][64:, :] = ss


def mid2_kernel(at_ref, a, b, c, d, *outs):
    x = at_ref[0]
    for k in range(4):
        for z in range(2):
            at = pl.multiple_of(z * 128 + ((x + k) % 4) * 32, 32)
            rows = pl.ds(at, 32)
            outs[k][z * 32 : z * 32 + 32, :] = (a[rows, :] + c[rows, :]) + (b[rows, :] + d[rows, :])


def last_kernel(at_ref, a1, b1, c1, d1, a2, b2, c2, d2, keep, send):
    z = at_ref[0]
    for out, half in ((keep, z), (send, 1 - z)):
        rows = pl.ds(pl.multiple_of(half * 32, 32), 32)
        out[:32, :] = (a1[rows, :] + c1[rows, :]) + (b1[rows, :] + d1[rows, :])
        out[32:64, :] = (a2[rows, :] + c2[rows, :]) + (b2[rows, :] + d2[rows, :])
        out[64:, :] = (a1[64:, :] + c1[64:, :]) + (b1[64:, :] + d1[64:, :])


def score_kernel(at_ref, keep, got, obs_ref, peak_ref):
    samples = 32 * ROWS
    factor = math.sqrt(samples - C - 2) / samples
    total = keep[...] + got[...]
    sums_e = jnp.concatenate([total[64:65, :], total[65:66, :128]], axis=1)
    scale_e = lax.rsqrt(sums_e / samples + EPSILON)
    lane = lax.broadcasted_iota(jnp.int32, (32, E), 1)
    row = lax.broadcasted_iota(jnp.int32, (32, E), 0)
    own = jnp.where(lane == row + at_ref[0] * 32, scale_e, 0.0)
    own_scale = jnp.sum(own, axis=1, keepdims=True)
    scale_v = lax.rsqrt(total[65:66, 128 : 128 + V] / samples + EPSILON)
    crosses = jnp.concatenate([total[:32, :], total[32:64, :]], axis=1)
    obs_ref[...] = crosses[:, :V] * own_scale * scale_v * factor
    place = lax.broadcasted_iota(jnp.int32, (32, 128), 1)
    peaks = jnp.zeros((32, 128), F32)
    for p in range(PERMS):
        part = crosses[:, (p + 1) * V : (p + 2) * V] * own_scale * scale_v * factor
        peaks = jnp.where(place == p, jnp.max(jnp.abs(part), axis=1, keepdims=True), peaks)
    peak_ref[...] = peaks


def peak_kernel(a, b, c, d, out_ref):
    best = jnp.maximum(jnp.maximum(a[...], b[...]), jnp.maximum(c[...], d[...]))
    full = jnp.concatenate([best, jnp.zeros((96, 128), F32)], axis=0)
    out_ref[...] = jnp.transpose(full)[:PERMS, :32]


def scalar_spec(n_in, n_out, grid=(1,)):
    whole = pl.BlockSpec(memory_space=pltpu.VMEM)
    return pltpu.PrefetchScalarGridSpec(
        num_scalar_prefetch=1,
        grid=grid,
        in_specs=[whole] * n_in,
        out_specs=[whole] * n_out,
    )


def index(axis):
    return jnp.reshape(lax.axis_index(axis), (1,)).astype(jnp.int32)


def shards(traits, covariates, genotypes, shuffles):
    core, x, y, zh = index("core"), index("x"), index("y"), index("zh")
    samp = (y * 2 + zh) * 4 + x
    whole = pl.BlockSpec(memory_space=pltpu.VMEM)

    pay, xt, dx = call(
        front_kernel,
        [((40, COLS), F32), ((48, ROWS), BF16), ((ROWS, V + 128), BF16)],
        core, traits, covariates, genotypes,
        grid_spec=pltpu.PrefetchScalarGridSpec(
            num_scalar_prefetch=1,
            grid=(1,),
            in_specs=[
                pl.BlockSpec((ROWS, HALF), lambda i, c: (0, c[0])),
                pl.BlockSpec((ROWS, C), lambda i, c: (0, 0)),
                pl.BlockSpec((ROWS, V), lambda i, c: (0, 0)),
            ],
            out_specs=[
                pl.BlockSpec((40, COLS), lambda i, c: (0, 0)),
                pl.BlockSpec((48, ROWS), lambda i, c: (0, 0)),
                pl.BlockSpec((ROWS, V + 128), lambda i, c: (0, 0)),
            ],
        ),
        flops=2 * 128 * ROWS * COLS,
        name="front",
    )
    yt = call(
        turn_kernel, [((E, ROWS), BF16)], traits,
        grid_spec=pl.GridSpec(
            grid=(4,),
            in_specs=[pl.BlockSpec((ROWS, 256), lambda i: (0, i))],
            out_specs=pl.BlockSpec((256, ROWS), lambda i: (i, 0)),
        ),
        flops=10**9,
        name="turn",
    )
    dxp = call(
        perm_kernel, [((PERMS, ROWS, V + 128), BF16)],
        samp * ROWS, shuffles.reshape(PERMS, 1, ROWS), dx,
        grid_spec=pltpu.PrefetchScalarGridSpec(
            num_scalar_prefetch=1,
            grid=(PERMS,),
            in_specs=[
                pl.BlockSpec((1, 1, ROWS), lambda i, b: (i, 0, 0)),
                pl.BlockSpec((ROWS, V + 128), lambda i, b: (0, 0)),
            ],
            out_specs=pl.BlockSpec((1, ROWS, V + 128), lambda i, b: (i, 0, 0)),
        ),
        flops=2 * PERMS * ROWS * ROWS * (V + 128),
        name="permute_rows",
    )

    pay = total_over(pay, "x")
    pay = total_over(pay, "y")
    coef = call(solve_kernel, [((40, V + HALF), F32)], pay, shift(pay, "zh", 1), name="solve", flops=10**8)
    far = shift(coef[:, V:], "core", 1)
    rt, g1, g2, ss = call(
        resid_kernel,
        [((E, ROWS), BF16), ((ROWS, CHUNK), BF16), ((ROWS, CHUNK), BF16), ((8, CHUNK), F32)],
        core, coef, far, yt, xt, dx, dxp,
        grid_spec=scalar_spec(6, 4),
        flops=2 * 2 * ROWS * E * 128,
        name="resid",
    )

    rt4 = rt.reshape(8, 4, 32, ROWS)
    g_spec = pl.BlockSpec((ROWS, CHUNK), lambda i, t: (0, 0))

    def cross1(k):
        return call(
            cross1_kernel, [((264, CHUNK), F32)], (x + k) % 4, rt4, g1, ss,
            grid_spec=pltpu.PrefetchScalarGridSpec(
                num_scalar_prefetch=1,
                grid=(1,),
                in_specs=[
                    pl.BlockSpec((8, 1, 32, ROWS), lambda i, t: (0, t[0], 0, 0)),
                    g_spec,
                    pl.BlockSpec((8, CHUNK), lambda i, t: (0, 0)),
                ],
                out_specs=pl.BlockSpec((264, CHUNK), lambda i, t: (0, 0)),
            ),
            flops=2 * 256 * ROWS * CHUNK,
            name=f"cross_x{k}",
        )

    def cross2(k):
        return call(
            cross2_kernel, [((256, CHUNK), F32)], (y + k) % 4, rt, g2,
            grid_spec=pltpu.PrefetchScalarGridSpec(
                num_scalar_prefetch=1,
                grid=(1,),
                in_specs=[pl.BlockSpec((256, ROWS), lambda i, t: (t[0], 0)), g_spec],
                out_specs=pl.BlockSpec((256, CHUNK), lambda i, t: (0, 0)),
            ),
            flops=2 * 256 * ROWS * CHUNK,
            name=f"cross_y{k}",
        )

    got1, got2 = {}, {}
    for k in (2, 1, 3):
        got1[k] = shift(cross1(k), "x", k)
        got2[k] = shift(cross2(k), "y", k)
    got1[0], got2[0] = cross1(0), cross2(0)

    parts1 = call(
        mid1_kernel, [((72, CHUNK), F32)] * 4, y, *(got1[k] for k in range(4)),
        grid_spec=scalar_spec(4, 4), flops=10**7, name="mid_x",
    )
    parts2 = call(
        mid2_kernel, [((64, CHUNK), F32)] * 4, x, *(got2[k] for k in range(4)),
        grid_spec=scalar_spec(4, 4), flops=10**7, name="mid_y",
    )
    fin1, fin2 = [parts1[0]], [parts2[0]]
    for k in (1, 2, 3):
        fin1.append(shift(parts1[k], "y", k))
        fin2.append(shift(parts2[k], "x", k))
    keep, send = call(
        last_kernel, [((72, CHUNK), F32)] * 2, zh, *fin1, *fin2,
        grid_spec=scalar_spec(8, 2), flops=10**6, name="last",
    )
    observed, peaks = call(
        score_kernel, [((32, V), F32), ((32, 128), F32)], samp, keep, shift(send, "zh", 1),
        grid_spec=scalar_spec(2, 2), flops=10**6, name="score",
    )
    peaks = jnp.maximum(peaks, shift(peaks, "core", 1))
    perm_max = call(
        peak_kernel, [((PERMS, 32), F32)], peaks, *(shift(peaks, "zl", k) for k in (1, 2, 3)),
        name="peak",
    )
    return observed, perm_max


def solution(mesh):
    fine = Mesh(mesh.devices.reshape(4, 2, 4, 4, 2), ("y", "zh", "x", "zl", "core"))
    samp, tile = ("y", "zh", "x"), ("zl", "core")
    return jax.shard_map(
        shards,
        mesh=fine,
        in_specs=(P(samp, None), P(samp, None), P(samp, tile), P(None, samp)),
        out_specs=(P(samp, tile), P(None, samp)),
        check_vma=False,
    )
```

```python
import math

import jax
import jax.numpy as jnp
from jax import lax
from jax.experimental import pallas as pl
from jax.experimental.pallas import tpu as pltpu
from jax.sharding import Mesh, PartitionSpec as P

C = 32
EPSILON = 1e-05

ROWS = 1024
E = 1024
V = 256
PERMS = 6
HALF = E // 2
COLS = V + HALF + 128
CHUNK = (PERMS + 1) * V // 2
F32 = jnp.float32
BF16 = jnp.bfloat16


def dot(a, b):
    return jnp.dot(a, b, preferred_element_type=F32)


def call(kernel, outs, *args, grid_spec=None, flops=0, name=None, room=4):
    shapes = [jax.ShapeDtypeStruct(s, d) for s, d in outs]
    single = len(shapes) == 1
    extra = {} if grid_spec is None else {"grid_spec": grid_spec}
    nbytes = sum(math.prod(s) * jnp.dtype(d).itemsize for s, d in outs)
    return pl.pallas_call(
        kernel,
        out_shape=shapes[0] if single else shapes,
        name=name,
        cost_estimate=pl.CostEstimate(flops=flops, bytes_accessed=nbytes, transcendentals=0),
        compiler_params=pltpu.CompilerParams(vmem_limit_bytes=room << 20),
        **extra,
    )(*args)


def shifts(axis, k):
    n = lax.axis_size(axis)
    return [(i, (i + k) % n) for i in range(n)]


def shift(value, axis, k):
    return lax.ppermute(value, axis, shifts(axis, k))


def total_over(value, axis):
    if lax.axis_size(axis) == 2:
        return value + shift(value, axis, 1)
    one, two, three = (shift(value, axis, k) for k in (1, 2, 3))
    return (value + two) + (one + three)


def front_kernel(core_ref, traits_ref, cov_ref, geno_ref, pay_ref, xt_ref, dx_ref):
    del core_ref
    row = lax.broadcasted_iota(jnp.int32, (128 - C, ROWS), 0)
    tail = jnp.where(row == 0, 1.0, 0.0).astype(F32)
    design_t = jnp.concatenate([cov_ref[...].astype(F32), tail], axis=0)
    dosage = geno_ref[...].astype(F32).astype(BF16)
    design_b = jnp.transpose(design_t).astype(BF16)
    dx_ref[:, :V] = dosage
    dx_ref[:, V:] = design_b
    xt = design_t[:48].astype(BF16)
    xt_ref[...] = xt
    pay_ref[:, :V] = dot(xt, dosage)[:40]
    pay_ref[:, V : V + HALF] = dot(xt, traits_ref[...])[:40]
    pay_ref[:, V + HALF :] = dot(xt, design_b)[:40]


def turn_kernel(traits_ref, out_ref):
    out_ref[...] = jnp.transpose(traits_ref[...])


def perm_kernel(base_ref, order_ref, dx_ref, out_ref):
    order = order_ref[0] - base_ref[0]
    for at in range(0, ROWS, 256):
        row = lax.broadcasted_iota(jnp.int32, (256, ROWS), 0) + at
        pick = jnp.where(row == order, 1.0, 0.0).astype(BF16)
        out_ref[0, at : at + 256, :] = dot(pick, dx_ref[...]).astype(BF16)


def solve_kernel(own_ref, far_ref, out_ref):
    m = own_ref[...] + far_ref[...]
    row_id = lax.broadcasted_iota(jnp.int32, (40, COLS), 0)
    for k in range(C + 1):
        at = V + HALF + k
        col = m[:, at : at + 1]
        row = m[k : k + 1, :] / m[k : k + 1, at : at + 1]
        m = jnp.where(row_id == k, row, m - col * row)
    out_ref[...] = m[:, : V + HALF]


def resid_kernel(core_ref, own_ref, far_ref, yt_ref, xt_ref, dx_ref, dxp_ref, rt_ref, g1_ref, g2_ref, ss_ref):
    core = core_ref[0]
    xt = xt_ref[...]
    zeros = jnp.zeros((8, E), F32)
    mine = own_ref[:, V:]
    other = far_ref[...]
    first = jnp.where(core == 0, mine, other)
    second = jnp.where(core == 0, other, mine)
    coef = jnp.concatenate([jnp.concatenate([first, second], axis=1), zeros], axis=0)
    coef_t = jnp.transpose(coef).astype(BF16)
    ss_parts = []
    for at in range(0, E, 128):
        res = yt_ref[at : at + 128, :].astype(F32) - dot(coef_t[at : at + 128], xt)
        rt_ref[at : at + 128, :] = res.astype(BF16)
        sq = res * res
        lanes = sq[:, :128]
        for b in range(128, ROWS, 128):
            lanes = lanes + sq[:, b : b + 128]
        ss_parts.append(jnp.sum(jnp.transpose(lanes), axis=0, keepdims=True))
    gamma = jnp.concatenate([own_ref[:, :V], jnp.zeros((88, V), F32)], axis=0).astype(BF16)
    res_g = dx_ref[:, :V].astype(F32) - dot(dx_ref[:, V:], gamma)
    g1_ref[:, :V] = res_g.astype(BF16)
    ss_v = jnp.sum(res_g * res_g, axis=0, keepdims=True)
    for p in range(PERMS):
        g = (dxp_ref[p, :, :V].astype(F32) - dot(dxp_ref[p, :, V:], gamma)).astype(BF16)
        at = (p + 1) * V
        if at + V <= CHUNK:
            g1_ref[:, at : at + V] = g
        elif at >= CHUNK:
            g2_ref[:, at - CHUNK : at - CHUNK + V] = g
        else:
            g1_ref[:, at:] = g[:, : CHUNK - at]
            g2_ref[:, : at + V - CHUNK] = g[:, CHUNK - at :]
    ss_ref[...] = jnp.zeros((8, CHUNK), F32)
    ss_ref[0:1, :] = jnp.concatenate(ss_parts[:7], axis=1)
    ss_ref[1:2, :128] = ss_parts[7]
    ss_ref[1:2, 128 : 128 + V] = ss_v


def cross1_kernel(to_ref, rt_ref, g_ref, ss_ref, out_ref):
    del to_ref
    rows = rt_ref[...].reshape(256, ROWS)
    out_ref[:256, :] = dot(rows, g_ref[...])
    out_ref[256:, :] = ss_ref[...]


def cross2_kernel(to_ref, rt_ref, g_ref, out_ref):
    del to_ref
    out_ref[...] = dot(rt_ref[...], g_ref[...])


def mid1_kernel(at_ref, a, b, c, d, *outs):
    y = at_ref[0]
    ss = (a[256:, :] + c[256:, :]) + (b[256:, :] + d[256:, :])
    for k in range(4):
        at = pl.multiple_of(((y + k) % 4) * 64, 64)
        rows = pl.ds(at, 64)
        outs[k][:64, :] = (a[rows, :] + c[rows, :]) + (b[rows, :] + d[rows, :])
        outs[k][64:, :] = ss


def mid2_kernel(at_ref, a, b, c, d, *outs):
    x = at_ref[0]
    for k in range(4):
        for z in range(2):
            at = pl.multiple_of(z * 128 + ((x + k) % 4) * 32, 32)
            rows = pl.ds(at, 32)
            outs[k][z * 32 : z * 32 + 32, :] = (a[rows, :] + c[rows, :]) + (b[rows, :] + d[rows, :])


def last_kernel(at_ref, a1, b1, c1, d1, a2, b2, c2, d2, keep, send):
    z = at_ref[0]
    for out, half in ((keep, z), (send, 1 - z)):
        rows = pl.ds(pl.multiple_of(half * 32, 32), 32)
        out[:32, :] = (a1[rows, :] + c1[rows, :]) + (b1[rows, :] + d1[rows, :])
        out[32:64, :] = (a2[rows, :] + c2[rows, :]) + (b2[rows, :] + d2[rows, :])
        out[64:, :] = (a1[64:, :] + c1[64:, :]) + (b1[64:, :] + d1[64:, :])


def score_kernel(at_ref, keep, got, obs_ref, peak_ref):
    samples = 32 * ROWS
    factor = math.sqrt(samples - C - 2) / samples
    total = keep[...] + got[...]
    sums_e = jnp.concatenate([total[64:65, :], total[65:66, :128]], axis=1)
    scale_e = lax.rsqrt(sums_e / samples + EPSILON)
    lane = lax.broadcasted_iota(jnp.int32, (32, E), 1)
    row = lax.broadcasted_iota(jnp.int32, (32, E), 0)
    own = jnp.where(lane == row + at_ref[0] * 32, scale_e, 0.0)
    own_scale = jnp.sum(own, axis=1, keepdims=True)
    scale_v = lax.rsqrt(total[65:66, 128 : 128 + V] / samples + EPSILON)
    crosses = jnp.concatenate([total[:32, :], total[32:64, :]], axis=1)
    obs_ref[...] = crosses[:, :V] * own_scale * scale_v * factor
    place = lax.broadcasted_iota(jnp.int32, (32, 128), 1)
    peaks = jnp.zeros((32, 128), F32)
    for p in range(PERMS):
        part = crosses[:, (p + 1) * V : (p + 2) * V] * own_scale * scale_v * factor
        peaks = jnp.where(place == p, jnp.max(jnp.abs(part), axis=1, keepdims=True), peaks)
    peak_ref[...] = peaks


def peak_kernel(a, b, c, d, out_ref):
    best = jnp.maximum(jnp.maximum(a[...], b[...]), jnp.maximum(c[...], d[...]))
    full = jnp.concatenate([best, jnp.zeros((96, 128), F32)], axis=0)
    out_ref[...] = jnp.transpose(full)[:PERMS, :32]


def scalar_spec(n_in, n_out, grid=(1,)):
    whole = pl.BlockSpec(memory_space=pltpu.VMEM)
    return pltpu.PrefetchScalarGridSpec(
        num_scalar_prefetch=1,
        grid=grid,
        in_specs=[whole] * n_in,
        out_specs=[whole] * n_out,
    )


def index(axis):
    return jnp.reshape(lax.axis_index(axis), (1,)).astype(jnp.int32)


def shards(traits, covariates, genotypes, shuffles):
    core, x, y, zh = index("core"), index("x"), index("y"), index("zh")
    samp = (y * 2 + zh) * 4 + x
    whole = pl.BlockSpec(memory_space=pltpu.VMEM)

    pay, xt, dx = call(
        front_kernel,
        [((40, COLS), F32), ((48, ROWS), BF16), ((ROWS, V + 128), BF16)],
        core, traits, covariates.T, genotypes,
        grid_spec=pltpu.PrefetchScalarGridSpec(
            num_scalar_prefetch=1,
            grid=(1,),
            in_specs=[
                pl.BlockSpec((ROWS, HALF), lambda i, c: (0, c[0])),
                pl.BlockSpec((C, ROWS), lambda i, c: (0, 0)),
                pl.BlockSpec((ROWS, V), lambda i, c: (0, 0)),
            ],
            out_specs=[
                pl.BlockSpec((40, COLS), lambda i, c: (0, 0)),
                pl.BlockSpec((48, ROWS), lambda i, c: (0, 0)),
                pl.BlockSpec((ROWS, V + 128), lambda i, c: (0, 0)),
            ],
        ),
        flops=2 * 128 * ROWS * COLS,
        name="front", room=14,
    )
    yt = call(
        turn_kernel, [((E, ROWS), BF16)], traits,
        grid_spec=pl.GridSpec(
            grid=(4,),
            in_specs=[pl.BlockSpec((ROWS, 256), lambda i: (0, i))],
            out_specs=pl.BlockSpec((256, ROWS), lambda i: (i, 0)),
        ),
        flops=10**9,
        name="turn", room=6,
    )
    dxp = call(
        perm_kernel, [((PERMS, ROWS, V + 128), BF16)],
        samp * ROWS, shuffles.reshape(PERMS, 1, ROWS), dx,
        grid_spec=pltpu.PrefetchScalarGridSpec(
            num_scalar_prefetch=1,
            grid=(PERMS,),
            in_specs=[
                pl.BlockSpec((1, 1, ROWS), lambda i, b: (i, 0, 0)),
                pl.BlockSpec((ROWS, V + 128), lambda i, b: (0, 0)),
            ],
            out_specs=pl.BlockSpec((1, ROWS, V + 128), lambda i, b: (i, 0, 0)),
        ),
        flops=2 * PERMS * ROWS * ROWS * (V + 128),
        name="permute_rows", room=10,
    )

    pay = total_over(pay, "x")
    pay = total_over(pay, "y")
    coef = call(solve_kernel, [((40, V + HALF), F32)], pay, shift(pay, "zh", 1), name="solve", room=4, flops=10**8)
    far = shift(coef[:, V:], "core", 1)
    rt, g1, g2, ss = call(
        resid_kernel,
        [((E, ROWS), BF16), ((ROWS, CHUNK), BF16), ((ROWS, CHUNK), BF16), ((8, CHUNK), F32)],
        core, coef, far, yt, xt, dx, dxp,
        grid_spec=scalar_spec(6, 4),
        flops=2 * 2 * ROWS * E * 128,
        name="resid", room=24,
    )

    rt4 = rt.reshape(8, 4, 32, ROWS)
    g_spec = pl.BlockSpec((ROWS, CHUNK), lambda i, t: (0, 0))

    def cross1(k):
        return call(
            cross1_kernel, [((264, CHUNK), F32)], (x + k) % 4, rt4, g1, ss,
            grid_spec=pltpu.PrefetchScalarGridSpec(
                num_scalar_prefetch=1,
                grid=(1,),
                in_specs=[
                    pl.BlockSpec((8, 1, 32, ROWS), lambda i, t: (0, t[0], 0, 0)),
                    g_spec,
                    pl.BlockSpec((8, CHUNK), lambda i, t: (0, 0)),
                ],
                out_specs=pl.BlockSpec((264, CHUNK), lambda i, t: (0, 0)),
            ),
            flops=2 * 256 * ROWS * CHUNK,
            name=f"cross_x{k}", room=10,
        )

    def cross2(k):
        return call(
            cross2_kernel, [((256, CHUNK), F32)], (y + k) % 4, rt, g2,
            grid_spec=pltpu.PrefetchScalarGridSpec(
                num_scalar_prefetch=1,
                grid=(1,),
                in_specs=[pl.BlockSpec((256, ROWS), lambda i, t: (t[0], 0)), g_spec],
                out_specs=pl.BlockSpec((256, CHUNK), lambda i, t: (0, 0)),
            ),
            flops=2 * 256 * ROWS * CHUNK,
            name=f"cross_y{k}", room=10,
        )

    got1, got2 = {}, {}
    for k in (2, 1, 3):
        got1[k] = shift(cross1(k), "x", k)
        got2[k] = shift(cross2(k), "y", k)
    got1[0], got2[0] = cross1(0), cross2(0)

    parts1 = call(
        mid1_kernel, [((72, CHUNK), F32)] * 4, y, *(got1[k] for k in range(4)),
        grid_spec=scalar_spec(4, 4), flops=10**7, name="mid_x", room=12,
    )
    parts2 = call(
        mid2_kernel, [((64, CHUNK), F32)] * 4, x, *(got2[k] for k in range(4)),
        grid_spec=scalar_spec(4, 4), flops=10**7, name="mid_y", room=12,
    )
    fin1, fin2 = [parts1[0]], [parts2[0]]
    for k in (1, 2, 3):
        fin1.append(shift(parts1[k], "y", k))
        fin2.append(shift(parts2[k], "x", k))
    keep, send = call(
        last_kernel, [((72, CHUNK), F32)] * 2, zh, *fin1, *fin2,
        grid_spec=scalar_spec(8, 2), flops=10**6, name="last", room=6,
    )
    observed, peaks = call(
        score_kernel, [((32, V), F32), ((32, 128), F32)], samp, keep, shift(send, "zh", 1),
        grid_spec=scalar_spec(2, 2), flops=10**6, name="score", room=4,
    )
    peaks = jnp.maximum(peaks, shift(peaks, "core", 1))
    perm_max = call(
        peak_kernel, [((PERMS, 32), F32)], peaks, *(shift(peaks, "zl", k) for k in (1, 2, 3)),
        name="peak", room=2,
    )
    return observed, perm_max


def solution(mesh):
    fine = Mesh(mesh.devices.reshape(4, 2, 4, 4, 2), ("y", "zh", "x", "zl", "core"))
    samp, tile = ("y", "zh", "x"), ("zl", "core")
    return jax.shard_map(
        shards,
        mesh=fine,
        in_specs=(P(samp, None), P(samp, None), P(samp, tile), P(None, samp)),
        out_specs=(P(samp, tile), P(None, samp)),
        check_vma=False,
    )
```

```python
import math

import jax
import jax.numpy as jnp
from jax import lax
from jax.experimental import pallas as pl
from jax.experimental.pallas import tpu as pltpu
from jax.sharding import Mesh, PartitionSpec as P

C = 32
EPSILON = 1e-05

ROWS = 1024
E = 1024
V = 256
PERMS = 6
HALF = E // 2
COLS = V + HALF + 128
BLOCKS = (V + HALF) // 128
CHUNK = (PERMS + 1) * V // 2
F32 = jnp.float32
BF16 = jnp.bfloat16


def dot(a, b):
    return jnp.dot(a, b, preferred_element_type=F32)


def call(kernel, outs, *args, grid_spec=None, in_specs=None, flops=0, name=None, room=4):
    shapes = [jax.ShapeDtypeStruct(s, d) for s, d in outs]
    single = len(shapes) == 1
    extra = {} if grid_spec is None else {"grid_spec": grid_spec}
    if in_specs is not None:
        extra["in_specs"] = in_specs
    nbytes = sum(math.prod(s) * jnp.dtype(d).itemsize for s, d in outs)
    out = pl.pallas_call(
        kernel,
        out_shape=shapes[0] if single else shapes,
        name=name,
        cost_estimate=pl.CostEstimate(flops=flops, bytes_accessed=nbytes, transcendentals=0),
        compiler_params=pltpu.CompilerParams(vmem_limit_bytes=room << 20),
        **extra,
    )(*args)
    return out if single else list(out)


def shifts(axis, k):
    n = lax.axis_size(axis)
    return [(i, (i + k) % n) for i in range(n)]


def shift(value, axis, k):
    return lax.ppermute(value, axis, shifts(axis, k))


def front_kernel(core_ref, traits_ref, cov_ref, geno_ref, pay_ref, xt_ref, dx_ref):
    del core_ref
    row = lax.broadcasted_iota(jnp.int32, (128 - C, ROWS), 0)
    tail = jnp.where(row == 0, 1.0, 0.0).astype(F32)
    design_t = jnp.concatenate([cov_ref[...].astype(F32), tail], axis=0)
    dosage = geno_ref[...].astype(F32).astype(BF16)
    design_b = jnp.transpose(design_t).astype(BF16)
    dx_ref[:, :V] = dosage
    dx_ref[:, V:] = design_b
    xt = design_t[:48].astype(BF16)
    xt_ref[...] = xt
    pay_ref[BLOCKS * C :, :] = dot(xt, design_b)[:40]
    for at, part in ((0, dot(xt, dosage)), (V // 128, dot(xt, traits_ref[...]))):
        for j in range(part.shape[1] // 128):
            block = part[:, j * 128 : (j + 1) * 128]
            pay_ref[(at + j) * C : (at + j + 1) * C, :] = block[:C]
            ones = BLOCKS * C + C + 1 + at + j
            pay_ref[ones : ones + 1, :] = block[C : C + 1]


def turn_kernel(traits_ref, out_ref):
    out_ref[...] = jnp.transpose(traits_ref[...])


def perm_kernel(base_ref, order_ref, dx_ref, after_ref, out_ref, token_ref):
    del after_ref
    order = order_ref[0] - base_ref[0]
    for at in range(0, ROWS, 256):
        row = lax.broadcasted_iota(jnp.int32, (256, ROWS), 0) + at
        pick = jnp.where(row == order, 1.0, 0.0).astype(BF16)
        out_ref[0, at : at + 256, :] = dot(pick, dx_ref[...]).astype(BF16)
    token_ref[...] = jnp.zeros(token_ref.shape, F32)


def sum_kernel(a, b, c, d, token, out):
    del token
    out[...] = (a[...] + c[...]) + (b[...] + d[...])


def solve_kernel(own_ref, far_ref, out_ref):
    total = own_ref[...] + far_ref[...]
    gram = total[BLOCKS * C :]
    blocks = [total[j * C : (j + 1) * C] for j in range(BLOCKS)]
    ones = [gram[C + 1 + j : C + 2 + j] for j in range(BLOCKS)]
    row_id = lax.broadcasted_iota(jnp.int32, (40, COLS), 0)
    top = jnp.concatenate([*blocks, gram[:C]], axis=1)
    low = jnp.concatenate([*ones, gram[C : C + 1]], axis=1)
    m = jnp.concatenate([top, jnp.broadcast_to(low, (8, COLS))], axis=0)
    for k in range(C + 1):
        at = V + HALF + k
        col = m[:, at : at + 1]
        row = m[k : k + 1, :] / m[k : k + 1, at : at + 1]
        m = jnp.where(row_id == k, row, m - col * row)
    out_ref[...] = jnp.where(row_id[:, : V + HALF] <= C, m[:, : V + HALF], 0.0)


def resid_kernel(core_ref, own_ref, far_ref, yt_ref, xt_ref, dx_ref, dxp1_ref, dxp2_ref, rt_ref, g1_ref, g2_ref, ss_ref):
    core = core_ref[0]
    xt = xt_ref[...]
    zeros = jnp.zeros((8, E), F32)
    mine = own_ref[:, V:]
    other = far_ref[...]
    first = jnp.where(core == 0, mine, other)
    second = jnp.where(core == 0, other, mine)
    coef = jnp.concatenate([jnp.concatenate([first, second], axis=1), zeros], axis=0)
    coef_t = jnp.transpose(coef).astype(BF16)
    ss_parts = []
    for at in range(0, E, 128):
        res = yt_ref[at : at + 128, :].astype(F32) - dot(coef_t[at : at + 128], xt)
        rt_ref[at : at + 128, :] = res.astype(BF16)
        sq = res * res
        lanes = sq[:, :128]
        for b in range(128, ROWS, 128):
            lanes = lanes + sq[:, b : b + 128]
        ss_parts.append(jnp.sum(jnp.transpose(lanes), axis=0, keepdims=True))
    gamma = jnp.concatenate([own_ref[:, :V], jnp.zeros((88, V), F32)], axis=0).astype(BF16)
    res_g = dx_ref[:, :V].astype(F32) - dot(dx_ref[:, V:], gamma)
    g1_ref[:, :V] = res_g.astype(BF16)
    ss_v = jnp.sum(res_g * res_g, axis=0, keepdims=True)
    for p in range(PERMS):
        src, q = (dxp1_ref, p) if p < PERMS // 2 else (dxp2_ref, p - PERMS // 2)
        g = (src[q, :, :V].astype(F32) - dot(src[q, :, V:], gamma)).astype(BF16)
        at = (p + 1) * V
        if at + V <= CHUNK:
            g1_ref[:, at : at + V] = g
        elif at >= CHUNK:
            g2_ref[:, at - CHUNK : at - CHUNK + V] = g
        else:
            g1_ref[:, at:] = g[:, : CHUNK - at]
            g2_ref[:, : at + V - CHUNK] = g[:, CHUNK - at :]
    ss_ref[...] = jnp.zeros((8, CHUNK), F32)
    ss_ref[0:1, :] = jnp.concatenate(ss_parts[:7], axis=1)
    ss_ref[1:2, :128] = ss_parts[7]
    ss_ref[1:2, 128 : 128 + V] = ss_v


def cross1_kernel(to_ref, rt_ref, g_ref, ss_ref, after_ref, low_ref, high_ref):
    del to_ref, after_ref
    low_ref[:128, :] = dot(rt_ref[:, 0, 0].reshape(128, ROWS), g_ref[...])
    low_ref[128:, :] = ss_ref[...]
    high_ref[...] = dot(rt_ref[:, 1, 0].reshape(128, ROWS), g_ref[...])


def cross2_kernel(to_ref, rt_ref, g_ref, after_ref, low_ref, high_ref):
    del to_ref, after_ref
    low_ref[...] = dot(rt_ref[:128], g_ref[...])
    high_ref[...] = dot(rt_ref[128:], g_ref[...])


def relay_kernel(a, b, after, out):
    del after
    out[...] = a[...] + b[...]


def mid_kernel(at_ref, low, low_near, low_far, high, high_near, high_far, *outs):
    me = at_ref[0]
    for k in range(4):
        rows = pl.ds(pl.multiple_of(((me + k) % 4) * 32, 32), 32)
        outs[k][:32, :] = low[rows, :] + (low_near[rows, :] + low_far[rows, :])
        outs[k][32:64, :] = high[rows, :] + (high_near[rows, :] + high_far[rows, :])
        if outs[k].shape[0] > 64:
            outs[k][64:, :] = low[128:, :] + (low_near[128:, :] + low_far[128:, :])


def last_kernel(at_ref, a, b, c, d, keep, send):
    z = at_ref[0]
    for out, half in ((keep, z), (send, 1 - z)):
        rows = pl.ds(pl.multiple_of(half * 32, 32), 32)
        out[:32, :] = (a[rows, :] + c[rows, :]) + (b[rows, :] + d[rows, :])
        if out.shape[0] > 32:
            out[32:, :] = (a[64:, :] + c[64:, :]) + (b[64:, :] + d[64:, :])


def score_kernel(at_ref, keep1, got1, keep2, got2, obs_ref, peak_ref):
    samples = 32 * ROWS
    factor = math.sqrt(samples - C - 2) / samples
    first = keep1[...] + got1[...]
    second = keep2[...] + got2[...]
    sums_e = jnp.concatenate([first[32:33, :], first[33:34, :128]], axis=1)
    scale_e = lax.rsqrt(sums_e / samples + EPSILON)
    lane = lax.broadcasted_iota(jnp.int32, (32, E), 1)
    row = lax.broadcasted_iota(jnp.int32, (32, E), 0)
    own = jnp.where(lane == row + at_ref[0] * 32, scale_e, 0.0)
    own_scale = jnp.sum(own, axis=1, keepdims=True)
    scale_v = lax.rsqrt(first[33:34, 128 : 128 + V] / samples + EPSILON)
    crosses = jnp.concatenate([first[:32, :], second], axis=1)
    obs_ref[...] = crosses[:, :V] * own_scale * scale_v * factor
    place = lax.broadcasted_iota(jnp.int32, (32, 128), 1)
    peaks = jnp.zeros((32, 128), F32)
    for p in range(PERMS):
        part = crosses[:, (p + 1) * V : (p + 2) * V] * own_scale * scale_v * factor
        peaks = jnp.where(place == p, jnp.max(jnp.abs(part), axis=1, keepdims=True), peaks)
    peak_ref[...] = peaks


def peak_kernel(a, b, c, d, out_ref):
    best = jnp.maximum(jnp.maximum(a[...], b[...]), jnp.maximum(c[...], d[...]))
    full = jnp.concatenate([best, jnp.zeros((96, 128), F32)], axis=0)
    out_ref[...] = jnp.transpose(full)[:PERMS, :32]


def scalar_spec(n_in, n_out, grid=(1,)):
    whole = pl.BlockSpec(memory_space=pltpu.VMEM)
    return pltpu.PrefetchScalarGridSpec(
        num_scalar_prefetch=1,
        grid=grid,
        in_specs=[whole] * n_in,
        out_specs=[whole] * n_out,
    )


def index(axis):
    return jnp.reshape(lax.axis_index(axis), (1,)).astype(jnp.int32)


def shards(traits, covariates, genotypes, shuffles):
    core, x, y, zh = index("core"), index("x"), index("y"), index("zh")
    samp = (y * 2 + zh) * 4 + x
    anywhere = pl.BlockSpec(memory_space=pl.ANY)

    pay, xt, dx = call(
        front_kernel,
        [((BLOCKS * C + 40, 128), F32), ((48, ROWS), BF16), ((ROWS, V + 128), BF16)],
        core, traits, covariates.T, genotypes,
        grid_spec=pltpu.PrefetchScalarGridSpec(
            num_scalar_prefetch=1,
            grid=(1,),
            in_specs=[
                pl.BlockSpec((ROWS, HALF), lambda i, c: (0, c[0])),
                pl.BlockSpec((C, ROWS), lambda i, c: (0, 0)),
                pl.BlockSpec((ROWS, V), lambda i, c: (0, 0)),
            ],
            out_specs=[
                pl.BlockSpec((BLOCKS * C + 40, 128), lambda i, c: (0, 0)),
                pl.BlockSpec((48, ROWS), lambda i, c: (0, 0)),
                pl.BlockSpec((ROWS, V + 128), lambda i, c: (0, 0)),
            ],
        ),
        flops=2 * 128 * ROWS * COLS,
        name="front", room=14,
    )

    def permuted(part, after):
        some = PERMS // 2
        return call(
            perm_kernel, [((some, ROWS, V + 128), BF16), ((8, 128), F32)],
            samp * ROWS, shuffles.reshape(PERMS, 1, ROWS), dx, after,
            grid_spec=pltpu.PrefetchScalarGridSpec(
                num_scalar_prefetch=1,
                grid=(some,),
                in_specs=[
                    pl.BlockSpec((1, 1, ROWS), lambda i, b: (i + part * some, 0, 0)),
                    pl.BlockSpec((ROWS, V + 128), lambda i, b: (0, 0)),
                    anywhere,
                ],
                out_specs=[
                    pl.BlockSpec((1, ROWS, V + 128), lambda i, b: (i, 0, 0)),
                    pl.BlockSpec((8, 128), lambda i, b: (0, 0)),
                ],
            ),
            flops=2 * some * ROWS * ROWS * (V + 128),
            name=f"permute_rows{part}", room=8,
        )

    def summed(value, axis, token):
        parts = [value] + [shift(value, axis, k) for k in (1, 2, 3)]
        return call(sum_kernel, [(value.shape, F32)], *parts, token, name=f"sum_{axis}", room=2)

    dxp1, token = permuted(0, pay)
    pay = summed(pay, "x", token)
    dxp2, token = permuted(1, pay)
    pay = summed(pay, "y", token)
    yt = call(
        turn_kernel, [((E, ROWS), BF16)], traits,
        grid_spec=pl.GridSpec(
            grid=(4,),
            in_specs=[pl.BlockSpec((ROWS, 256), lambda i: (0, i))],
            out_specs=pl.BlockSpec((256, ROWS), lambda i: (i, 0)),
        ),
        flops=10**9,
        name="turn", room=6,
    )
    coef = call(solve_kernel, [((40, V + HALF), F32)], pay, shift(pay, "zh", 1), name="solve", room=4, flops=10**8)
    far = shift(coef[:, V:], "core", 1)
    rt, g1, g2, ss = call(
        resid_kernel,
        [((E, ROWS), BF16), ((ROWS, CHUNK), BF16), ((ROWS, CHUNK), BF16), ((8, CHUNK), F32)],
        core, coef, far, yt, xt, dx, dxp1, dxp2,
        grid_spec=scalar_spec(7, 4),
        flops=2 * 2 * ROWS * E * 128,
        name="resid", room=24,
    )

    rt5 = rt.reshape(4, 2, 4, 32, ROWS)
    g_spec = pl.BlockSpec((ROWS, CHUNK), lambda i, t: (0, 0))
    ss_spec = pl.BlockSpec((8, CHUNK), lambda i, t: (0, 0))

    def cross(axis, k, after):
        onx = axis == "x"
        low = 136 if onx else 128
        return call(
            cross1_kernel if onx else cross2_kernel,
            [((low, CHUNK), F32), ((128, CHUNK), F32)],
            ((x if onx else y) + k) % 4,
            *((rt5, g1, ss) if onx else (rt, g2)),
            after,
            grid_spec=pltpu.PrefetchScalarGridSpec(
                num_scalar_prefetch=1,
                grid=(1,),
                in_specs=[
                    *(
                        (pl.BlockSpec((4, 2, 1, 32, ROWS), lambda i, t: (0, 0, t[0], 0, 0)), g_spec, ss_spec)
                        if onx
                        else (pl.BlockSpec((256, ROWS), lambda i, t: (t[0], 0)), g_spec)
                    ),
                    anywhere,
                ],
                out_specs=[
                    pl.BlockSpec((low, CHUNK), lambda i, t: (0, 0)),
                    pl.BlockSpec((128, CHUNK), lambda i, t: (0, 0)),
                ],
            ),
            flops=2 * 256 * ROWS * CHUNK,
            name=f"cross_{axis}{k}", room=10,
        )

    part, got = {}, {}
    after = ss
    for k in (2, 1, 3, 0):
        for axis in ("x", "y"):
            part[axis, k] = cross(axis, k, after)
            after = part[axis, k][1]
            low, high = part[axis, k]
            if k == 2:
                got[axis, "low2"], got[axis, "high2"] = shift(low, axis, 1), shift(high, axis, 3)
            elif k == 1:
                got[axis, "high"] = shift(high, axis, 1)
            elif k == 3:
                got[axis, "low"] = shift(low, axis, 3)
    parts = {}
    whole = pl.BlockSpec(memory_space=pltpu.VMEM)
    for axis in ("x", "y"):
        relayed = []
        for k, half, name in ((1, 0, "low2"), (3, 1, "high2")):
            mine = part[axis, k][half]
            relayed.append(
                call(
                    relay_kernel, [(mine.shape, F32)], mine, got[axis, name], after,
                    in_specs=[whole, whole, anywhere], name=f"relay_{axis}{k}", room=2,
                )
            )
        got[axis, "lows"], got[axis, "highs"] = shift(relayed[0], axis, 1), shift(relayed[1], axis, 3)
    keeps = []
    for axis, other, at in (("x", "y", y), ("y", "x", x)):
        rows = 72 if axis == "x" else 64
        low, high = part[axis, 0]
        parts[axis] = call(
            mid_kernel, [((rows, CHUNK), F32)] * 4, at,
            low, got[axis, "low"], got[axis, "lows"], high, got[axis, "high"], got[axis, "highs"],
            grid_spec=scalar_spec(6, 4), flops=10**7, name=f"mid_{axis}", room=4,
        )
        for k in (1, 2, 3):
            parts[axis][k] = shift(parts[axis][k], other, k)
    for axis in ("x", "y"):
        rows = 40 if axis == "x" else 32
        keep, send = call(
            last_kernel, [((rows, CHUNK), F32)] * 2, zh, *parts[axis],
            grid_spec=scalar_spec(4, 2), flops=10**6, name=f"last_{axis}", room=2,
        )
        keeps += [keep, shift(send, "zh", 1)]
    observed, peaks = call(
        score_kernel, [((32, V), F32), ((32, 128), F32)], samp, *keeps,
        grid_spec=scalar_spec(4, 2), flops=10**6, name="score", room=4,
    )
    peaks = jnp.maximum(peaks, shift(peaks, "core", 1))
    perm_max = call(
        peak_kernel, [((PERMS, 32), F32)], peaks, *(shift(peaks, "zl", k) for k in (1, 2, 3)),
        name="peak", room=2,
    )
    return observed, perm_max


def solution(mesh):
    fine = Mesh(mesh.devices.reshape(4, 2, 4, 4, 2), ("y", "zh", "x", "zl", "core"))
    samp, tile = ("y", "zh", "x"), ("zl", "core")
    return jax.shard_map(
        shards,
        mesh=fine,
        in_specs=(P(samp, None), P(samp, None), P(samp, tile), P(None, samp)),
        out_specs=(P(samp, tile), P(None, samp)),
        check_vma=False,
    )
```

```python
import math

import jax
import jax.numpy as jnp
from jax import lax
from jax.experimental import pallas as pl
from jax.experimental.pallas import tpu as pltpu
from jax.sharding import Mesh, PartitionSpec as P


C = 32
EPSILON = 1e-05

ROWS = 1024
E = 1024
V = 256
PERMS = 6
HALF = E // 2
COLS = V + HALF + 128
BLOCKS = (V + HALF) // 128
SPLIT = (3, 2, 1)
SQUARES = 16
CHUNK = (PERMS + 1) * V // 2
LANES = CHUNK // 128
F32 = jnp.float32
BF16 = jnp.bfloat16


def dot(a, b):
    return jnp.dot(a, b, preferred_element_type=F32)


def call(kernel, outs, *args, grid_spec=None, in_specs=None, flops=0, room=4):
    shapes = [jax.ShapeDtypeStruct(s, d) for s, d in outs]
    single = len(shapes) == 1
    extra = {} if grid_spec is None else {"grid_spec": grid_spec}
    if in_specs is not None:
        extra["in_specs"] = in_specs
    nbytes = sum(math.prod(s) * jnp.dtype(d).itemsize for s, d in outs)
    out = pl.pallas_call(
        kernel,
        out_shape=shapes[0] if single else shapes,
        cost_estimate=pl.CostEstimate(flops=flops, bytes_accessed=nbytes, transcendentals=0),
        compiler_params=pltpu.CompilerParams(vmem_limit_bytes=room << 20),
        **extra,
    )(*args)
    return out if single else list(out)


def shifts(axis, k):
    n = lax.axis_size(axis)
    return [(i, (i + k) % n) for i in range(n)]


def shift(value, axis, k):
    return lax.ppermute(value, axis, shifts(axis, k))


def front_kernel(core_ref, traits_ref, cov_ref, geno_ref, pay_ref, xt_ref, dx_ref):
    del core_ref
    row = lax.broadcasted_iota(jnp.int32, (128 - C, ROWS), 0)
    tail = jnp.where(row == 0, 1.0, 0.0).astype(F32)
    design_t = jnp.concatenate([cov_ref[...].astype(F32), tail], axis=0)
    dosage = geno_ref[...].astype(F32).astype(BF16)
    design_b = jnp.transpose(design_t).astype(BF16)
    dx_ref[:, :V] = dosage
    dx_ref[:, V:] = design_b
    xt = design_t[:48].astype(BF16)
    xt_ref[...] = xt
    pay_ref[BLOCKS * C :, :] = dot(xt, design_b)[:40]
    for at, part in ((0, dot(xt, dosage)), (V // 128, dot(xt, traits_ref[...]))):
        for j in range(part.shape[1] // 128):
            block = part[:, j * 128 : (j + 1) * 128]
            pay_ref[(at + j) * C : (at + j + 1) * C, :] = block[:C]
            ones = BLOCKS * C + C + 1 + at + j
            pay_ref[ones : ones + 1, :] = block[C : C + 1]


def turn_kernel(traits_ref, out_ref):
    out_ref[...] = jnp.transpose(traits_ref[...])


def perm_kernel(base_ref, order_ref, dx_ref, after_ref, out_ref, token_ref):
    del after_ref
    order = order_ref[0] - base_ref[0]
    for at in range(0, ROWS, 256):
        row = lax.broadcasted_iota(jnp.int32, (256, ROWS), 0) + at
        pick = jnp.where(row == order, 1.0, 0.0).astype(BF16)
        out_ref[0, at : at + 256, :] = dot(pick, dx_ref[...]).astype(BF16)
    token_ref[...] = jnp.zeros(token_ref.shape, F32)


def sum_kernel(a, b, c, d, token, out):
    del token
    out[...] = (a[...] + c[...]) + (b[...] + d[...])


def solve_kernel(own_ref, far_ref, out_ref):
    total = own_ref[...] + far_ref[...]
    gram = total[BLOCKS * C :]
    blocks = [total[j * C : (j + 1) * C] for j in range(BLOCKS)]
    ones = [gram[C + 1 + j : C + 2 + j] for j in range(BLOCKS)]
    row_id = lax.broadcasted_iota(jnp.int32, (40, COLS), 0)
    top = jnp.concatenate([*blocks, gram[:C]], axis=1)
    low = jnp.concatenate([*ones, gram[C : C + 1]], axis=1)
    m = jnp.concatenate([top, jnp.broadcast_to(low, (8, COLS))], axis=0)
    for k in range(C + 1):
        at = V + HALF + k
        col = m[:, at : at + 1]
        row = m[k : k + 1, :] / m[k : k + 1, at : at + 1]
        m = jnp.where(row_id == k, row, m - col * row)
    out_ref[...] = jnp.where(row_id[:, : V + HALF] <= C, m[:, : V + HALF], 0.0)


def resid_kernel(core_ref, own_ref, far_ref, yt_ref, xt_ref, dx_ref, dxp1_ref, dxp2_ref, dxp3_ref, rt_ref, g1_ref, g2_ref, ss_ref):
    core = core_ref[0]
    xt = xt_ref[...]
    zeros = jnp.zeros((8, E), F32)
    mine = own_ref[:, V:]
    other = far_ref[...]
    first = jnp.where(core == 0, mine, other)
    second = jnp.where(core == 0, other, mine)
    coef = jnp.concatenate([jnp.concatenate([first, second], axis=1), zeros], axis=0)
    coef_t = jnp.transpose(coef).astype(BF16)
    ss_parts = []
    for at in range(0, E, 128):
        res = yt_ref[at : at + 128, :].astype(F32) - dot(coef_t[at : at + 128], xt)
        rt_ref[at : at + 128, :] = res.astype(BF16)
        sq = res * res
        lanes = sq[:, :128]
        for b in range(128, ROWS, 128):
            lanes = lanes + sq[:, b : b + 128]
        ss_parts.append(jnp.sum(jnp.transpose(lanes), axis=0, keepdims=True))
    gamma = jnp.concatenate([own_ref[:, :V], jnp.zeros((88, V), F32)], axis=0).astype(BF16)
    res_g = dx_ref[:, :V].astype(F32) - dot(dx_ref[:, V:], gamma)
    g1_ref[:, :V] = res_g.astype(BF16)
    ss_v = jnp.sum(res_g * res_g, axis=0, keepdims=True)
    places = [(ref, q) for ref in (dxp1_ref, dxp2_ref, dxp3_ref) for q in range(ref.shape[0])]
    for p, (src, q) in enumerate(places):
        g = (src[q, :, :V].astype(F32) - dot(src[q, :, V:], gamma)).astype(BF16)
        at = (p + 1) * V
        if at + V <= CHUNK:
            g1_ref[:, at : at + V] = g
        elif at >= CHUNK:
            g2_ref[:, at - CHUNK : at - CHUNK + V] = g
        else:
            g1_ref[:, at:] = g[:, : CHUNK - at]
            g2_ref[:, : at + V - CHUNK] = g[:, CHUNK - at :]
    ss_ref[...] = jnp.concatenate(
        [*ss_parts, ss_v[:, :128], ss_v[:, 128:], jnp.zeros((SQUARES - 10, 128), F32)], axis=0
    )


def lanes_to_rows(out_ref, value):
    rows = value.shape[0]
    for j in range(LANES):
        out_ref[j * rows : (j + 1) * rows, :] = value[:, j * 128 : (j + 1) * 128]


def cross1_kernel(to_ref, rt_ref, g_ref, ss_ref, after_ref, low_ref, high_ref):
    del to_ref, after_ref
    lanes_to_rows(low_ref, dot(rt_ref[:, 0, 0].reshape(128, ROWS), g_ref[...]))
    low_ref[LANES * 128 :, :] = ss_ref[...]
    lanes_to_rows(high_ref, dot(rt_ref[:, 1, 0].reshape(128, ROWS), g_ref[...]))


def cross2_kernel(to_ref, rt_ref, g_ref, after_ref, low_ref, high_ref):
    del to_ref, after_ref
    lanes_to_rows(low_ref, dot(rt_ref[:128], g_ref[...]))
    lanes_to_rows(high_ref, dot(rt_ref[128:], g_ref[...]))


def relay_kernel(a, b, after, out):
    del after
    out[...] = a[...] + b[...]


def mid_kernel(at_ref, low, low_near, low_far, high, high_near, high_far, *outs):
    me = at_ref[0]
    for k in range(4):
        for j in range(LANES):
            rows = pl.ds(pl.multiple_of(j * 128 + ((me + k) % 4) * 32, 32), 32)
            outs[k][j * 64 : j * 64 + 32, :] = low[rows, :] + (low_near[rows, :] + low_far[rows, :])
            outs[k][j * 64 + 32 : j * 64 + 64, :] = high[rows, :] + (high_near[rows, :] + high_far[rows, :])
        if outs[k].shape[0] > LANES * 64:
            rows = pl.ds(LANES * 128, SQUARES)
            outs[k][LANES * 64 :, :] = low[rows, :] + (low_near[rows, :] + low_far[rows, :])


def last_kernel(at_ref, a, b, c, d, keep, send):
    z = at_ref[0]
    for out, half in ((keep, z), (send, 1 - z)):
        for j in range(LANES):
            rows = pl.ds(pl.multiple_of(j * 64 + half * 32, 32), 32)
            out[j * 32 : (j + 1) * 32, :] = (a[rows, :] + c[rows, :]) + (b[rows, :] + d[rows, :])
        if out.shape[0] > LANES * 32:
            rows = pl.ds(LANES * 64, SQUARES)
            out[LANES * 32 :, :] = (a[rows, :] + c[rows, :]) + (b[rows, :] + d[rows, :])


def score_kernel(at_ref, keep1, got1, keep2, got2, obs_ref, peak_ref):
    samples = 32 * ROWS
    factor = math.sqrt(samples - C - 2) / samples
    first = keep1[...] + got1[...]
    second = keep2[...] + got2[...]
    sums = first[LANES * 32 :]
    scales = lax.rsqrt(sums / samples + EPSILON)
    place = lax.broadcasted_iota(jnp.int32, (SQUARES, 128), 0)
    lane = lax.broadcasted_iota(jnp.int32, (32, 128), 1)
    row = lax.broadcasted_iota(jnp.int32, (32, 128), 0)
    scale_e = jnp.sum(jnp.where(place == at_ref[0] // 4, scales, 0.0), axis=0, keepdims=True)
    own = jnp.where(lane == row + (at_ref[0] % 4) * 32, scale_e, 0.0)
    own_scale = jnp.sum(own, axis=1, keepdims=True)
    scale_v = jnp.concatenate([scales[8:9], scales[9:10]], axis=1)
    blocks = [part[j * 32 : (j + 1) * 32] for part in (first, second) for j in range(LANES)]

    def scores(p):
        cross = jnp.concatenate([blocks[2 * p], blocks[2 * p + 1]], axis=1)
        return cross * own_scale * scale_v * factor

    obs_ref[...] = scores(0)
    peaks = jnp.zeros((32, 128), F32)
    for p in range(PERMS):
        peaks = jnp.where(lane == p, jnp.max(jnp.abs(scores(p + 1)), axis=1, keepdims=True), peaks)
    peak_ref[...] = peaks


def peak_kernel(a, b, c, d, out_ref):
    best = jnp.maximum(jnp.maximum(a[...], b[...]), jnp.maximum(c[...], d[...]))
    full = jnp.concatenate([best, jnp.zeros((96, 128), F32)], axis=0)
    out_ref[...] = jnp.transpose(full)[:PERMS, :32]


def scalar_spec(n_in, n_out, grid=(1,)):
    whole = pl.BlockSpec(memory_space=pltpu.VMEM)
    return pltpu.PrefetchScalarGridSpec(
        num_scalar_prefetch=1,
        grid=grid,
        in_specs=[whole] * n_in,
        out_specs=[whole] * n_out,
    )


def in_hbm(value):
    return pltpu.with_memory_space_constraint(value, pltpu.HBM)


def index(axis):
    return jnp.reshape(lax.axis_index(axis), (1,)).astype(jnp.int32)


def program(traits, covariates, genotypes, shuffles):
    core, x, y, zh = index("core"), index("x"), index("y"), index("zh")
    samp = (y * 2 + zh) * 4 + x
    anywhere = pl.BlockSpec(memory_space=pl.ANY)

    pay, xt, dx = call(
        front_kernel,
        [((BLOCKS * C + 40, 128), F32), ((48, ROWS), BF16), ((ROWS, V + 128), BF16)],
        core, in_hbm(traits), in_hbm(covariates.T), in_hbm(genotypes),
        grid_spec=pltpu.PrefetchScalarGridSpec(
            num_scalar_prefetch=1,
            grid=(1,),
            in_specs=[
                pl.BlockSpec((ROWS, HALF), lambda i, c: (0, c[0])),
                pl.BlockSpec((C, ROWS), lambda i, c: (0, 0)),
                pl.BlockSpec((ROWS, V), lambda i, c: (0, 0)),
            ],
            out_specs=[
                pl.BlockSpec((BLOCKS * C + 40, 128), lambda i, c: (0, 0)),
                pl.BlockSpec((48, ROWS), lambda i, c: (0, 0)),
                pl.BlockSpec((ROWS, V + 128), lambda i, c: (0, 0)),
            ],
        ),
        flops=2 * 128 * ROWS * COLS,
        room=14,
    )

    orders = shuffles.reshape(PERMS, 1, ROWS)

    def permuted(first, count, after):
        return call(
            perm_kernel, [((count, ROWS, V + 128), BF16), ((8, 128), F32)],
            samp * ROWS, orders, dx, after,
            grid_spec=pltpu.PrefetchScalarGridSpec(
                num_scalar_prefetch=1,
                grid=(count,),
                in_specs=[
                    pl.BlockSpec((1, 1, ROWS), lambda i, b: (i + first, 0, 0)),
                    pl.BlockSpec((ROWS, V + 128), lambda i, b: (0, 0)),
                    anywhere,
                ],
                out_specs=[
                    pl.BlockSpec((1, ROWS, V + 128), lambda i, b: (i, 0, 0)),
                    pl.BlockSpec((8, 128), lambda i, b: (0, 0)),
                ],
            ),
            flops=2 * count * ROWS * ROWS * (V + 128),
            room=8,
        )

    def summed(value, axis, token):
        parts = [value] + [shift(value, axis, k) for k in (1, 2, 3)]
        return call(sum_kernel, [(value.shape, F32)], *parts, token, room=2)

    turned, at = [], 0
    for axis, count in (("x", SPLIT[0]), ("y", SPLIT[1])):
        rows, token = permuted(at, count, pay)
        pay = summed(pay, axis, token)
        turned.append(rows)
        at += count
    turned.append(permuted(at, SPLIT[2], pay)[0])
    yt = call(
        turn_kernel, [((E, ROWS), BF16)], traits,
        grid_spec=pl.GridSpec(
            grid=(4,),
            in_specs=[pl.BlockSpec((ROWS, 256), lambda i: (0, i))],
            out_specs=pl.BlockSpec((256, ROWS), lambda i: (i, 0)),
        ),
        flops=10**9,
        room=6,
    )
    coef = call(solve_kernel, [((40, V + HALF), F32)], pay, shift(pay, "zh", 1), room=4, flops=10**8)
    far = shift(coef[:, V:], "core", 1)
    rt, g1, g2, ss = call(
        resid_kernel,
        [((E, ROWS), BF16), ((ROWS, CHUNK), BF16), ((ROWS, CHUNK), BF16), ((SQUARES, 128), F32)],
        core, coef, far, yt, xt, dx, *turned,
        grid_spec=scalar_spec(8, 4),
        flops=2 * 2 * ROWS * E * 128,
        room=24,
    )

    rt5 = rt.reshape(4, 2, 4, 32, ROWS)
    g_spec = pl.BlockSpec((ROWS, CHUNK), lambda i, t: (0, 0))
    ss_spec = pl.BlockSpec((SQUARES, 128), lambda i, t: (0, 0))

    def cross(axis, k, after):
        onx = axis == "x"
        low = LANES * 128 + (SQUARES if onx else 0)
        return call(
            cross1_kernel if onx else cross2_kernel,
            [((low, 128), F32), ((LANES * 128, 128), F32)],
            ((x if onx else y) + k) % 4,
            *((rt5, g1, ss) if onx else (rt, g2)),
            after,
            grid_spec=pltpu.PrefetchScalarGridSpec(
                num_scalar_prefetch=1,
                grid=(1,),
                in_specs=[
                    *(
                        (pl.BlockSpec((4, 2, 1, 32, ROWS), lambda i, t: (0, 0, t[0], 0, 0)), g_spec, ss_spec)
                        if onx
                        else (pl.BlockSpec((256, ROWS), lambda i, t: (t[0], 0)), g_spec)
                    ),
                    anywhere,
                ],
                out_specs=[
                    pl.BlockSpec((low, 128), lambda i, t: (0, 0)),
                    pl.BlockSpec((LANES * 128, 128), lambda i, t: (0, 0)),
                ],
            ),
            flops=2 * 256 * ROWS * CHUNK,
            room=10,
        )

    part, got = {}, {}
    after = ss
    for k in (2, 1, 3, 0):
        for axis in ("x", "y"):
            part[axis, k] = cross(axis, k, after)
            after = part[axis, k][1]
            low, high = part[axis, k]
            if k == 2:
                got[axis, "low2"] = shift(low, axis, 1)
                got[axis, "high2"] = shift(high, axis, 3)
            elif k == 1:
                got[axis, "high"] = shift(high, axis, 1)
            elif k == 3:
                got[axis, "low"] = shift(low, axis, 3)
    parts = {}
    whole = pl.BlockSpec(memory_space=pltpu.VMEM)
    for axis in ("x", "y"):
        relayed = []
        for k, half, name in ((1, 0, "low2"), (3, 1, "high2")):
            mine = part[axis, k][half]
            relayed.append(
                call(
                    relay_kernel, [(mine.shape, F32)], mine, got[axis, name], after,
                    in_specs=[whole, whole, anywhere], room=2,
                )
            )
        got[axis, "lows"], got[axis, "highs"] = shift(relayed[0], axis, 1), shift(relayed[1], axis, 3)
    keeps = []
    for axis, other, at in (("x", "y", y), ("y", "x", x)):
        rows = LANES * 64 + (SQUARES if axis == "x" else 0)
        low, high = part[axis, 0]
        parts[axis] = call(
            mid_kernel, [((rows, 128), F32)] * 4, at,
            low, got[axis, "low"], got[axis, "lows"], high, got[axis, "high"], got[axis, "highs"],
            grid_spec=scalar_spec(6, 4), flops=10**7, room=4,
        )
        for k in (1, 2, 3):
            parts[axis][k] = shift(parts[axis][k], other, k)
    for axis in ("x", "y"):
        rows = LANES * 32 + (SQUARES if axis == "x" else 0)
        keep, send = call(
            last_kernel, [((rows, 128), F32)] * 2, zh, *parts[axis],
            grid_spec=scalar_spec(4, 2), flops=10**6, room=2,
        )
        keeps += [keep, shift(send, "zh", 1)]
    observed, peaks = call(
        score_kernel, [((32, V), F32), ((32, 128), F32)], samp, *keeps,
        grid_spec=scalar_spec(4, 2), flops=10**6, room=4,
    )
    peaks = jnp.maximum(peaks, shift(peaks, "core", 1))
    perm_max = call(
        peak_kernel, [((PERMS, 32), F32)], peaks, *(shift(peaks, "zl", k) for k in (1, 2, 3)),
        room=2,
    )
    return observed, perm_max


def solution(mesh):
    fine = Mesh(mesh.devices.reshape(4, 2, 4, 4, 2), ("y", "zh", "x", "zl", "core"))
    samp, tile = ("y", "zh", "x"), ("zl", "core")
    return jax.shard_map(
        program,
        mesh=fine,
        in_specs=(P(samp, None), P(samp, None), P(samp, tile), P(None, samp)),
        out_specs=(P(samp, tile), P(None, samp)),
        check_vma=False,
    )
```

```python
import math

import jax
import jax.numpy as jnp
from jax import lax
from jax.experimental import pallas as pl
from jax.experimental.pallas import tpu as pltpu
from jax.sharding import Mesh, PartitionSpec as P


C = 32
EPSILON = 1e-05

ROWS = 1024
E = 1024
V = 256
PERMS = 6
HALF = E // 2
COLS = V + HALF + 128
BLOCKS = (V + HALF) // 128
SPLIT = (3, 2, 1)
SQUARES = 16
CHUNK = (PERMS + 1) * V // 2
LANES = CHUNK // 128
F32 = jnp.float32
BF16 = jnp.bfloat16


def dot(a, b):
    return jnp.dot(a, b, preferred_element_type=F32)


def call(kernel, outs, *args, grid_spec=None, in_specs=None, flops=0, room=4):
    shapes = [jax.ShapeDtypeStruct(s, d) for s, d in outs]
    single = len(shapes) == 1
    extra = {} if grid_spec is None else {"grid_spec": grid_spec}
    if in_specs is not None:
        extra["in_specs"] = in_specs
    nbytes = sum(math.prod(s) * jnp.dtype(d).itemsize for s, d in outs)
    out = pl.pallas_call(
        kernel,
        out_shape=shapes[0] if single else shapes,
        cost_estimate=pl.CostEstimate(flops=flops, bytes_accessed=nbytes, transcendentals=0),
        compiler_params=pltpu.CompilerParams(vmem_limit_bytes=room << 20),
        **extra,
    )(*args)
    return out if single else list(out)


def shifts(axis, k):
    n = lax.axis_size(axis)
    return [(i, (i + k) % n) for i in range(n)]


def shift(value, axis, k):
    return lax.ppermute(value, axis, shifts(axis, k))


def front_kernel(core_ref, traits_ref, cov_ref, geno_ref, pay_ref, xt_ref, dx_ref):
    del core_ref
    row = lax.broadcasted_iota(jnp.int32, (128 - C, ROWS), 0)
    tail = jnp.where(row == 0, 1.0, 0.0).astype(F32)
    design_t = jnp.concatenate([cov_ref[...].astype(F32), tail], axis=0)
    dosage = geno_ref[...].astype(F32).astype(BF16)
    design_b = jnp.transpose(design_t).astype(BF16)
    dx_ref[:, :V] = dosage
    dx_ref[:, V:] = design_b
    xt = design_t[:48].astype(BF16)
    xt_ref[...] = xt
    pay_ref[BLOCKS * C :, :] = dot(xt, design_b)[:40]
    for at, part in ((0, dot(xt, dosage)), (V // 128, dot(xt, traits_ref[...]))):
        for j in range(part.shape[1] // 128):
            block = part[:, j * 128 : (j + 1) * 128]
            pay_ref[(at + j) * C : (at + j + 1) * C, :] = block[:C]
            ones = BLOCKS * C + C + 1 + at + j
            pay_ref[ones : ones + 1, :] = block[C : C + 1]


def turn_kernel(traits_ref, out_ref):
    out_ref[...] = jnp.transpose(traits_ref[...])


def perm_kernel(base_ref, order_ref, dx_ref, after_ref, out_ref, token_ref):
    del after_ref
    order = order_ref[0] - base_ref[0]
    for at in range(0, ROWS, 256):
        row = lax.broadcasted_iota(jnp.int32, (256, ROWS), 0) + at
        pick = jnp.where(row == order, 1.0, 0.0).astype(BF16)
        out_ref[0, at : at + 256, :] = dot(pick, dx_ref[...]).astype(BF16)
    token_ref[...] = jnp.zeros(token_ref.shape, F32)


def sum_kernel(a, b, c, d, token, out):
    del token
    out[...] = (a[...] + c[...]) + (b[...] + d[...])


def solve_kernel(own_ref, far_ref, out_ref):
    total = own_ref[...] + far_ref[...]
    base = BLOCKS * C
    m = [
        [total[j * C + g * 8 : j * C + g * 8 + 8] for j in range(BLOCKS)] + [total[base + g * 8 : base + g * 8 + 8]]
        for g in range(C // 8)
    ]
    wide = (8, 128)
    zero = jnp.broadcast_to(total[base + 39 : base + 40], wide)
    ones = [total[base + C + 1 + j : base + C + 2 + j] for j in range(BLOCKS)] + [total[base + C : base + C + 1]]
    m.append([jnp.broadcast_to(part, wide) for part in ones])
    row_id = lax.broadcasted_iota(jnp.int32, wide, 0)

    def line_of(part, line):
        return jnp.broadcast_to(part[line : line + 1], wide)

    for k in range(0, C, 2):
        here, line = k // 8, k % 8
        left = [jnp.broadcast_to(part[BLOCKS][:, k : k + 1], wide) + zero for part in m]
        right = [jnp.broadcast_to(part[BLOCKS][:, k + 1 : k + 2], wide) + zero for part in m]
        p, q = line_of(left[here], line), line_of(right[here], line)
        r, s = line_of(left[here], line + 1), line_of(right[here], line + 1)
        inverse = 1.0 / (p * s - q * r)
        p, q, r, s = p * inverse, q * inverse, r * inverse, s * inverse
        for j in range(BLOCKS + 1):
            top, low = line_of(m[here][j], line), line_of(m[here][j], line + 1)
            top, low = s * top - q * low, p * low - r * top
            for g in range(len(m)):
                rest = m[g][j] - left[g] * top - right[g] * low
                if g == here:
                    rest = jnp.where(row_id == line, top, jnp.where(row_id == line + 1, low, rest))
                m[g][j] = rest
    last = [jnp.broadcast_to(part[BLOCKS][:, C : C + 1], wide) + zero for part in m]
    inverse = 1.0 / line_of(last[-1], 0)
    for j in range(BLOCKS):
        row = line_of(m[-1][j], 0) * inverse
        for g in range(len(m)):
            m[g][j] = m[g][j] - last[g] * row if g < C // 8 else row
    for g in range(len(m)):
        for j in range(BLOCKS):
            done = m[g][j] if g < C // 8 else jnp.where(row_id == 0, m[g][j], 0.0)
            out_ref[g * 8 : g * 8 + 8, j * 128 : (j + 1) * 128] = done


def geno_kernel(own_ref, dx_ref, dxp1_ref, dxp2_ref, dxp3_ref, g1_ref, g2_ref, ss_ref):
    gamma = jnp.concatenate([own_ref[:, :V], jnp.zeros((88, V), F32)], axis=0).astype(BF16)
    res_g = dx_ref[:, :V].astype(F32) - dot(dx_ref[:, V:], gamma)
    g1_ref[:, :V] = res_g.astype(BF16)
    ss_v = jnp.sum(res_g * res_g, axis=0, keepdims=True)
    ss_ref[...] = jnp.concatenate([ss_v[:, :128], ss_v[:, 128:], jnp.zeros((6, 128), F32)], axis=0)
    places = [(ref, q) for ref in (dxp1_ref, dxp2_ref, dxp3_ref) for q in range(ref.shape[0])]
    for p, (src, q) in enumerate(places):
        g = (src[q, :, :V].astype(F32) - dot(src[q, :, V:], gamma)).astype(BF16)
        at = (p + 1) * V
        if at + V <= CHUNK:
            g1_ref[:, at : at + V] = g
        elif at >= CHUNK:
            g2_ref[:, at - CHUNK : at - CHUNK + V] = g
        else:
            g1_ref[:, at:] = g[:, : CHUNK - at]
            g2_ref[:, : at + V - CHUNK] = g[:, CHUNK - at :]


def resid_kernel(core_ref, own_ref, far_ref, yt_ref, xt_ref, ss_v_ref, rt_ref, ss_ref):
    core = core_ref[0]
    xt = xt_ref[...]
    mine = own_ref[:, V:]
    other = far_ref[...]
    first = jnp.where(core == 0, mine, other)
    second = jnp.where(core == 0, other, mine)
    coef = jnp.concatenate([jnp.concatenate([first, second], axis=1), jnp.zeros((8, E), F32)], axis=0)
    coef_t = jnp.transpose(coef).astype(BF16)
    for j in range(E // 128):
        at = j * 128
        res = yt_ref[at : at + 128, :].astype(F32) - dot(coef_t[at : at + 128], xt)
        rt_ref[at : at + 128, :] = res.astype(BF16)
        sq = res * res
        lanes = sq[:, :128]
        for b in range(128, ROWS, 128):
            lanes = lanes + sq[:, b : b + 128]
        ss_ref[j : j + 1, :] = jnp.sum(jnp.transpose(lanes), axis=0, keepdims=True)
    ss_ref[8:, :] = ss_v_ref[...]


def lanes_to_rows(out_ref, value):
    rows = value.shape[0]
    for j in range(LANES):
        out_ref[j * rows : (j + 1) * rows, :] = value[:, j * 128 : (j + 1) * 128]


def cross1_kernel(to_ref, rt_ref, g_ref, ss_ref, after_ref, low_ref, high_ref):
    del to_ref, after_ref
    lanes_to_rows(low_ref, dot(rt_ref[:, 0, 0].reshape(128, ROWS), g_ref[...]))
    low_ref[LANES * 128 :, :] = ss_ref[...]
    lanes_to_rows(high_ref, dot(rt_ref[:, 1, 0].reshape(128, ROWS), g_ref[...]))


def cross2_kernel(to_ref, rt_ref, g_ref, after_ref, low_ref, high_ref):
    del to_ref, after_ref
    lanes_to_rows(low_ref, dot(rt_ref[:128], g_ref[...]))
    lanes_to_rows(high_ref, dot(rt_ref[128:], g_ref[...]))


def relay_kernel(a, b, after, out):
    del after
    out[...] = a[...] + b[...]


def mid_kernel(at_ref, low, low_near, low_far, high, high_near, high_far, *outs):
    me = at_ref[0]
    for k in range(4):
        for j in range(LANES):
            rows = pl.ds(pl.multiple_of(j * 128 + ((me + k) % 4) * 32, 32), 32)
            outs[k][j * 64 : j * 64 + 32, :] = low[rows, :] + (low_near[rows, :] + low_far[rows, :])
            outs[k][j * 64 + 32 : j * 64 + 64, :] = high[rows, :] + (high_near[rows, :] + high_far[rows, :])
        if outs[k].shape[0] > LANES * 64:
            rows = pl.ds(LANES * 128, SQUARES)
            outs[k][LANES * 64 :, :] = low[rows, :] + (low_near[rows, :] + low_far[rows, :])


def last_kernel(at_ref, a, b, c, d, keep, send):
    z = at_ref[0]
    for out, half in ((keep, z), (send, 1 - z)):
        for j in range(LANES):
            rows = pl.ds(pl.multiple_of(j * 64 + half * 32, 32), 32)
            out[j * 32 : (j + 1) * 32, :] = (a[rows, :] + c[rows, :]) + (b[rows, :] + d[rows, :])
        if out.shape[0] > LANES * 32:
            rows = pl.ds(LANES * 64, SQUARES)
            out[LANES * 32 :, :] = (a[rows, :] + c[rows, :]) + (b[rows, :] + d[rows, :])


FACTOR = math.sqrt(32 * ROWS - C - 2) / (32 * ROWS)


def score1_kernel(at_ref, keep, got, obs_ref, peak_ref, scale_ref):
    total = keep[...] + got[...]
    scales = lax.rsqrt(total[LANES * 32 :] / (32 * ROWS) + EPSILON)
    place = lax.broadcasted_iota(jnp.int32, (SQUARES, 128), 0)
    lane = lax.broadcasted_iota(jnp.int32, (32, 128), 1)
    row = lax.broadcasted_iota(jnp.int32, (32, 128), 0)
    scale_e = jnp.sum(jnp.where(place == at_ref[0] // 4, scales, 0.0), axis=0, keepdims=True)
    own = jnp.where(lane == row + (at_ref[0] % 4) * 32, scale_e, 0.0)
    own_scale = jnp.broadcast_to(jnp.sum(own, axis=1, keepdims=True), (32, 128))
    scale_ref[:32, :] = own_scale
    scale_ref[32:, :] = scales[8:16]
    scale_v = [scales[8:9], scales[9:10]]
    peaks = [None] * 3
    for j in range(LANES):
        score = total[j * 32 : (j + 1) * 32] * own_scale * scale_v[j % 2] * FACTOR
        if j < 2:
            obs_ref[:, j * 128 : (j + 1) * 128] = score
        else:
            p = j // 2 - 1
            peaks[p] = jnp.abs(score) if peaks[p] is None else jnp.maximum(peaks[p], jnp.abs(score))
    out = jnp.zeros((32, 128), F32)
    for p, part in enumerate(peaks):
        out = jnp.where(lane == p, jnp.max(part, axis=1, keepdims=True), out)
    peak_ref[...] = out


def score2_kernel(keep, got, peak1_ref, scale_ref, peak_ref):
    total = keep[...] + got[...]
    own_scale = scale_ref[:32]
    scale_v = [scale_ref[32:33], scale_ref[33:34]]
    lane = lax.broadcasted_iota(jnp.int32, (32, 128), 1)
    peaks = [None] * PERMS
    for j in range(LANES):
        score = jnp.abs(total[j * 32 : (j + 1) * 32] * own_scale * scale_v[(j + LANES) % 2] * FACTOR)
        p = (j + LANES) // 2 - 1
        peaks[p] = score if peaks[p] is None else jnp.maximum(peaks[p], score)
    out = peak1_ref[...]
    for p, part in enumerate(peaks):
        if part is not None:
            best = jnp.max(part, axis=1, keepdims=True)
            out = jnp.where(lane == p, jnp.maximum(out, best), out)
    peak_ref[...] = out


def peak_kernel(a, b, c, d, out_ref):
    best = jnp.maximum(jnp.maximum(a[...], b[...]), jnp.maximum(c[...], d[...]))
    full = jnp.concatenate([best, jnp.zeros((96, 128), F32)], axis=0)
    out_ref[...] = jnp.transpose(full)[:PERMS, :32]


def scalar_spec(n_in, n_out, grid=(1,)):
    whole = pl.BlockSpec(memory_space=pltpu.VMEM)
    return pltpu.PrefetchScalarGridSpec(
        num_scalar_prefetch=1,
        grid=grid,
        in_specs=[whole] * n_in,
        out_specs=[whole] * n_out,
    )


def in_hbm(value):
    return pltpu.with_memory_space_constraint(value, pltpu.HBM)


def index(axis):
    return jnp.reshape(lax.axis_index(axis), (1,)).astype(jnp.int32)


def program(traits, covariates, genotypes, shuffles):
    core, x, y, zh = index("core"), index("x"), index("y"), index("zh")
    samp = (y * 2 + zh) * 4 + x
    anywhere = pl.BlockSpec(memory_space=pl.ANY)

    pay, xt, dx = call(
        front_kernel,
        [((BLOCKS * C + 40, 128), F32), ((48, ROWS), BF16), ((ROWS, V + 128), BF16)],
        core, in_hbm(traits), in_hbm(covariates.T), in_hbm(genotypes),
        grid_spec=pltpu.PrefetchScalarGridSpec(
            num_scalar_prefetch=1,
            grid=(1,),
            in_specs=[
                pl.BlockSpec((ROWS, HALF), lambda i, c: (0, c[0])),
                pl.BlockSpec((C, ROWS), lambda i, c: (0, 0)),
                pl.BlockSpec((ROWS, V), lambda i, c: (0, 0)),
            ],
            out_specs=[
                pl.BlockSpec((BLOCKS * C + 40, 128), lambda i, c: (0, 0)),
                pl.BlockSpec((48, ROWS), lambda i, c: (0, 0)),
                pl.BlockSpec((ROWS, V + 128), lambda i, c: (0, 0)),
            ],
        ),
        flops=2 * 128 * ROWS * COLS,
        room=14,
    )

    orders = shuffles.reshape(PERMS, 1, ROWS)

    def permuted(first, count, after):
        return call(
            perm_kernel, [((count, ROWS, V + 128), BF16), ((8, 128), F32)],
            samp * ROWS, orders, dx, after,
            grid_spec=pltpu.PrefetchScalarGridSpec(
                num_scalar_prefetch=1,
                grid=(count,),
                in_specs=[
                    pl.BlockSpec((1, 1, ROWS), lambda i, b: (i + first, 0, 0)),
                    pl.BlockSpec((ROWS, V + 128), lambda i, b: (0, 0)),
                    anywhere,
                ],
                out_specs=[
                    pl.BlockSpec((1, ROWS, V + 128), lambda i, b: (i, 0, 0)),
                    pl.BlockSpec((8, 128), lambda i, b: (0, 0)),
                ],
            ),
            flops=2 * count * ROWS * ROWS * (V + 128),
            room=8,
        )

    def summed(value, axis, token):
        parts = [value] + [shift(value, axis, k) for k in (1, 2, 3)]
        return call(sum_kernel, [(value.shape, F32)], *parts, token, room=2)

    turned, at = [], 0
    for axis, count in (("x", SPLIT[0]), ("y", SPLIT[1])):
        rows, token = permuted(at, count, pay)
        pay = summed(pay, axis, token)
        turned.append(rows)
        at += count
    turned.append(permuted(at, SPLIT[2], pay)[0])
    yt = call(
        turn_kernel, [((E, ROWS), BF16)], traits,
        grid_spec=pl.GridSpec(
            grid=(4,),
            in_specs=[pl.BlockSpec((ROWS, 256), lambda i: (0, i))],
            out_specs=pl.BlockSpec((256, ROWS), lambda i: (i, 0)),
        ),
        flops=10**9,
        room=6,
    )
    coef = call(solve_kernel, [((40, V + HALF), F32)], pay, shift(pay, "zh", 1), room=4, flops=10**8)
    far = shift(coef[:, V:], "core", 1)
    g1, g2, ss_v = call(
        geno_kernel,
        [((ROWS, CHUNK), BF16), ((ROWS, CHUNK), BF16), ((8, 128), F32)],
        coef, dx, *turned,
        flops=2 * 128 * ROWS * 2 * CHUNK,
        room=16,
    )
    rt, ss = call(
        resid_kernel,
        [((E, ROWS), BF16), ((SQUARES, 128), F32)],
        core, coef, far, yt, xt, ss_v,
        grid_spec=scalar_spec(5, 2),
        flops=2 * 128 * ROWS * E,
        room=12,
    )

    rt5 = rt.reshape(4, 2, 4, 32, ROWS)
    g_spec = pl.BlockSpec((ROWS, CHUNK), lambda i, t: (0, 0))
    ss_spec = pl.BlockSpec((SQUARES, 128), lambda i, t: (0, 0))

    def cross(axis, k, after):
        onx = axis == "x"
        low = LANES * 128 + (SQUARES if onx else 0)
        return call(
            cross1_kernel if onx else cross2_kernel,
            [((low, 128), F32), ((LANES * 128, 128), F32)],
            ((x if onx else y) + k) % 4,
            *((rt5, g1, ss) if onx else (rt, g2)),
            after,
            grid_spec=pltpu.PrefetchScalarGridSpec(
                num_scalar_prefetch=1,
                grid=(1,),
                in_specs=[
                    *(
                        (pl.BlockSpec((4, 2, 1, 32, ROWS), lambda i, t: (0, 0, t[0], 0, 0)), g_spec, ss_spec)
                        if onx
                        else (pl.BlockSpec((256, ROWS), lambda i, t: (t[0], 0)), g_spec)
                    ),
                    anywhere,
                ],
                out_specs=[
                    pl.BlockSpec((low, 128), lambda i, t: (0, 0)),
                    pl.BlockSpec((LANES * 128, 128), lambda i, t: (0, 0)),
                ],
            ),
            flops=2 * 256 * ROWS * CHUNK,
            room=10,
        )

    part, got = {}, {}
    after = ss
    for k in (2, 1, 3, 0):
        for axis in ("x", "y"):
            part[axis, k] = cross(axis, k, after)
            after = part[axis, k][1]
            low, high = part[axis, k]
            if k == 2:
                got[axis, "low2"] = shift(low, axis, 1)
                got[axis, "high2"] = shift(high, axis, 3)
            elif k == 1:
                got[axis, "high"] = shift(high, axis, 1)
            elif k == 3:
                got[axis, "low"] = shift(low, axis, 3)
    parts = {}
    whole = pl.BlockSpec(memory_space=pltpu.VMEM)
    for axis in ("x", "y"):
        relayed = []
        for k, half, name in ((1, 0, "low2"), (3, 1, "high2")):
            mine = part[axis, k][half]
            relayed.append(
                call(
                    relay_kernel, [(mine.shape, F32)], mine, got[axis, name], after,
                    in_specs=[whole, whole, anywhere], room=2,
                )
            )
        got[axis, "lows"] = shift(relayed[0], axis, 1)
        got[axis, "highs"] = shift(relayed[1], axis, 3)
    keeps = []
    for axis, other, at in (("x", "y", y), ("y", "x", x)):
        rows = LANES * 64 + (SQUARES if axis == "x" else 0)
        low, high = part[axis, 0]
        parts[axis] = call(
            mid_kernel, [((rows, 128), F32)] * 4, at,
            low, got[axis, "low"], got[axis, "lows"], high, got[axis, "high"], got[axis, "highs"],
            grid_spec=scalar_spec(6, 4), flops=10**7, room=4,
        )
        for k in (1, 2, 3):
            parts[axis][k] = shift(parts[axis][k], other, k)
    for axis in ("x", "y"):
        rows = LANES * 32 + (SQUARES if axis == "x" else 0)
        keep, send = call(
            last_kernel, [((rows, 128), F32)] * 2, zh, *parts[axis],
            grid_spec=scalar_spec(4, 2), flops=10**6, room=2,
        )
        keeps.append((keep, shift(send, "zh", 1)))
    observed, peaks, scales = call(
        score1_kernel, [((32, V), F32), ((32, 128), F32), ((40, 128), F32)], samp, *keeps[0],
        grid_spec=scalar_spec(2, 3), flops=10**6, room=4,
    )
    peaks = call(score2_kernel, [((32, 128), F32)], *keeps[1], peaks, scales, flops=10**6, room=4)
    peaks = jnp.maximum(peaks, shift(peaks, "core", 1))
    perm_max = call(
        peak_kernel, [((PERMS, 32), F32)], peaks, *(shift(peaks, "zl", k) for k in (1, 2, 3)),
        room=2,
    )
    return observed, perm_max


def solution(mesh):
    fine = Mesh(mesh.devices.reshape(4, 2, 4, 4, 2), ("y", "zh", "x", "zl", "core"))
    samp, tile = ("y", "zh", "x"), ("zl", "core")
    return jax.shard_map(
        program,
        mesh=fine,
        in_specs=(P(samp, None), P(samp, None), P(samp, tile), P(None, samp)),
        out_specs=(P(samp, tile), P(None, samp)),
        check_vma=False,
    )
```

```python
import math

import jax
import jax.numpy as jnp
from jax import lax
from jax.experimental import pallas as pl
from jax.experimental.pallas import tpu as pltpu
from jax.sharding import Mesh, PartitionSpec as P


C = 32
EPSILON = 1e-05

ROWS = 1024
E = 1024
V = 256
PERMS = 6
HALF = E // 2
COLS = V + HALF + 128
BLOCKS = (V + HALF) // 128
SPLIT = (3, 2, 1)
SQUARES = 16
CHUNK = (PERMS + 1) * V // 2
LANES = CHUNK // 128
F32 = jnp.float32
BF16 = jnp.bfloat16


def dot(a, b):
    return jnp.dot(a, b, preferred_element_type=F32)


def call(kernel, outs, *args, grid_spec=None, in_specs=None, flops=0, room=4):
    shapes = [jax.ShapeDtypeStruct(s, d) for s, d in outs]
    single = len(shapes) == 1
    extra = {} if grid_spec is None else {"grid_spec": grid_spec}
    if in_specs is not None:
        extra["in_specs"] = in_specs
    nbytes = sum(math.prod(s) * jnp.dtype(d).itemsize for s, d in outs)
    out = pl.pallas_call(
        kernel,
        out_shape=shapes[0] if single else shapes,
        cost_estimate=pl.CostEstimate(flops=flops, bytes_accessed=nbytes, transcendentals=0),
        compiler_params=pltpu.CompilerParams(vmem_limit_bytes=room << 20),
        **extra,
    )(*args)
    return out if single else list(out)


def shifts(axis, k):
    n = lax.axis_size(axis)
    return [(i, (i + k) % n) for i in range(n)]


def shift(value, axis, k):
    return lax.ppermute(value, axis, shifts(axis, k))


def front_kernel(core_ref, traits_ref, cov_ref, geno_ref, pay_ref, xt_ref, dx_ref):
    del core_ref
    row = lax.broadcasted_iota(jnp.int32, (128 - C, ROWS), 0)
    tail = jnp.where(row == 0, 1.0, 0.0).astype(F32)
    design_t = jnp.concatenate([cov_ref[...].astype(F32), tail], axis=0)
    dosage = geno_ref[...].astype(F32).astype(BF16)
    design_b = jnp.transpose(design_t).astype(BF16)
    dx_ref[:, :V] = dosage
    dx_ref[:, V:] = design_b
    xt = design_t[:48].astype(BF16)
    xt_ref[...] = xt
    pay_ref[BLOCKS * C :, :] = dot(xt, design_b)[:40]
    for at, part in ((0, dot(xt, dosage)), (V // 128, dot(xt, traits_ref[...]))):
        for j in range(part.shape[1] // 128):
            block = part[:, j * 128 : (j + 1) * 128]
            pay_ref[(at + j) * C : (at + j + 1) * C, :] = block[:C]
            ones = BLOCKS * C + C + 1 + at + j
            pay_ref[ones : ones + 1, :] = block[C : C + 1]


def turn_kernel(traits_ref, out_ref):
    out_ref[...] = jnp.transpose(traits_ref[...])


def perm_kernel(base_ref, order_ref, dx_ref, after_ref, out_ref, token_ref):
    del after_ref
    order = order_ref[0] - base_ref[0]
    for at in range(0, ROWS, 256):
        row = lax.broadcasted_iota(jnp.int32, (256, ROWS), 0) + at
        pick = jnp.where(row == order, 1.0, 0.0).astype(BF16)
        out_ref[0, at : at + 256, :] = dot(pick, dx_ref[...]).astype(BF16)
    token_ref[...] = jnp.zeros(token_ref.shape, F32)


def sum_kernel(a, b, c, d, token, out):
    del token
    out[...] = (a[...] + c[...]) + (b[...] + d[...])


def solve_kernel(own_ref, far_ref, out_ref):
    total = own_ref[...] + far_ref[...]
    base = BLOCKS * C
    m = [
        [total[j * C + g * 8 : j * C + g * 8 + 8] for j in range(BLOCKS)] + [total[base + g * 8 : base + g * 8 + 8]]
        for g in range(C // 8)
    ]
    wide = (8, 128)
    zero = jnp.broadcast_to(total[base + 39 : base + 40], wide)
    ones = [total[base + C + 1 + j : base + C + 2 + j] for j in range(BLOCKS)] + [total[base + C : base + C + 1]]
    m.append([jnp.broadcast_to(part, wide) for part in ones])
    row_id = lax.broadcasted_iota(jnp.int32, wide, 0)

    def line_of(part, line):
        return jnp.broadcast_to(part[line : line + 1], wide)

    ones = [jnp.broadcast_to(part[BLOCKS][:, C : C + 1], wide) + zero for part in m]
    inverse = 1.0 / line_of(ones[-1], 0)
    for j in range(BLOCKS + 1):
        row = line_of(m[-1][j], 0) * inverse
        for g in range(len(m)):
            m[g][j] = m[g][j] - ones[g] * row if g < C // 8 else row
    for k in range(0, C, 2):
        here, line = k // 8, k % 8
        left = [jnp.broadcast_to(part[BLOCKS][:, k : k + 1], wide) + zero for part in m]
        right = [jnp.broadcast_to(part[BLOCKS][:, k + 1 : k + 2], wide) + zero for part in m]
        p, q = line_of(left[here], line), line_of(right[here], line)
        r, s = line_of(left[here], line + 1), line_of(right[here], line + 1)
        inverse = 1.0 / (p * s - q * r)
        p, q, r, s = p * inverse, q * inverse, r * inverse, s * inverse
        for j in range(BLOCKS + 1):
            top, low = line_of(m[here][j], line), line_of(m[here][j], line + 1)
            top, low = s * top - q * low, p * low - r * top
            for g in range(len(m)):
                rest = m[g][j] - left[g] * top - right[g] * low
                if g == here:
                    rest = jnp.where(row_id == line, top, jnp.where(row_id == line + 1, low, rest))
                m[g][j] = rest
    for g in range(len(m)):
        for j in range(BLOCKS):
            done = m[g][j] if g < C // 8 else jnp.where(row_id == 0, m[g][j], 0.0)
            out_ref[g * 8 : g * 8 + 8, j * 128 : (j + 1) * 128] = done


def geno_kernel(own_ref, dx_ref, dxp1_ref, dxp2_ref, dxp3_ref, g1_ref, g2_ref, ss_ref):
    gamma = jnp.concatenate([own_ref[:, :V], jnp.zeros((88, V), F32)], axis=0).astype(BF16)
    res_g = dx_ref[:, :V].astype(F32) - dot(dx_ref[:, V:], gamma)
    g1_ref[:, :V] = res_g.astype(BF16)
    ss_v = jnp.sum(res_g * res_g, axis=0, keepdims=True)
    ss_ref[...] = jnp.concatenate([ss_v[:, :128], ss_v[:, 128:], jnp.zeros((6, 128), F32)], axis=0)
    places = [(ref, q) for ref in (dxp1_ref, dxp2_ref, dxp3_ref) for q in range(ref.shape[0])]
    for p, (src, q) in enumerate(places):
        g = (src[q, :, :V].astype(F32) - dot(src[q, :, V:], gamma)).astype(BF16)
        at = (p + 1) * V
        if at + V <= CHUNK:
            g1_ref[:, at : at + V] = g
        elif at >= CHUNK:
            g2_ref[:, at - CHUNK : at - CHUNK + V] = g
        else:
            g1_ref[:, at:] = g[:, : CHUNK - at]
            g2_ref[:, : at + V - CHUNK] = g[:, CHUNK - at :]


def resid_kernel(core_ref, own_ref, far_ref, yt_ref, xt_ref, ss_v_ref, rt_ref, ss_ref):
    core = core_ref[0]
    xt = xt_ref[...]
    mine = own_ref[:, V:]
    other = far_ref[...]
    first = jnp.where(core == 0, mine, other)
    second = jnp.where(core == 0, other, mine)
    coef = jnp.concatenate([jnp.concatenate([first, second], axis=1), jnp.zeros((8, E), F32)], axis=0)
    coef_t = jnp.transpose(coef).astype(BF16)
    for j in range(E // 128):
        at = j * 128
        res = yt_ref[at : at + 128, :].astype(F32) - dot(coef_t[at : at + 128], xt)
        rt_ref[at : at + 128, :] = res.astype(BF16)
        sq = res * res
        lanes = sq[:, :128]
        for b in range(128, ROWS, 128):
            lanes = lanes + sq[:, b : b + 128]
        ss_ref[j : j + 1, :] = jnp.sum(jnp.transpose(lanes), axis=0, keepdims=True)
    ss_ref[8:, :] = ss_v_ref[...]


def lanes_to_rows(out_ref, value):
    rows = value.shape[0]
    for j in range(LANES):
        out_ref[j * rows : (j + 1) * rows, :] = value[:, j * 128 : (j + 1) * 128]


def cross1_kernel(to_ref, rt_ref, g_ref, ss_ref, after_ref, low_ref, high_ref):
    del to_ref, after_ref
    lanes_to_rows(low_ref, dot(rt_ref[:, 0, 0].reshape(128, ROWS), g_ref[...]))
    low_ref[LANES * 128 :, :] = ss_ref[...]
    lanes_to_rows(high_ref, dot(rt_ref[:, 1, 0].reshape(128, ROWS), g_ref[...]))


def cross2_kernel(to_ref, rt_ref, g_ref, after_ref, low_ref, high_ref):
    del to_ref, after_ref
    lanes_to_rows(low_ref, dot(rt_ref[:128], g_ref[...]))
    lanes_to_rows(high_ref, dot(rt_ref[128:], g_ref[...]))


def relay_kernel(a, b, after, out):
    del after
    out[...] = a[...] + b[...]


def mid_kernel(at_ref, low, low_near, low_far, high, high_near, high_far, *outs):
    me = at_ref[0]
    for k in range(4):
        for j in range(LANES):
            rows = pl.ds(pl.multiple_of(j * 128 + ((me + k) % 4) * 32, 32), 32)
            outs[k][j * 64 : j * 64 + 32, :] = low[rows, :] + (low_near[rows, :] + low_far[rows, :])
            outs[k][j * 64 + 32 : j * 64 + 64, :] = high[rows, :] + (high_near[rows, :] + high_far[rows, :])
        if outs[k].shape[0] > LANES * 64:
            rows = pl.ds(LANES * 128, SQUARES)
            outs[k][LANES * 64 :, :] = low[rows, :] + (low_near[rows, :] + low_far[rows, :])


def last_kernel(at_ref, a, b, c, d, keep, send):
    z = at_ref[0]
    for out, half in ((keep, z), (send, 1 - z)):
        for j in range(LANES):
            rows = pl.ds(pl.multiple_of(j * 64 + half * 32, 32), 32)
            out[j * 32 : (j + 1) * 32, :] = (a[rows, :] + c[rows, :]) + (b[rows, :] + d[rows, :])
        if out.shape[0] > LANES * 32:
            rows = pl.ds(LANES * 64, SQUARES)
            out[LANES * 32 :, :] = (a[rows, :] + c[rows, :]) + (b[rows, :] + d[rows, :])


FACTOR = math.sqrt(32 * ROWS - C - 2) / (32 * ROWS)


def score1_kernel(at_ref, keep, got, obs_ref, peak_ref, scale_ref):
    total = keep[...] + got[...]
    scales = lax.rsqrt(total[LANES * 32 :] / (32 * ROWS) + EPSILON)
    place = lax.broadcasted_iota(jnp.int32, (SQUARES, 128), 0)
    lane = lax.broadcasted_iota(jnp.int32, (32, 128), 1)
    row = lax.broadcasted_iota(jnp.int32, (32, 128), 0)
    scale_e = jnp.sum(jnp.where(place == at_ref[0] // 4, scales, 0.0), axis=0, keepdims=True)
    own = jnp.where(lane == row + (at_ref[0] % 4) * 32, scale_e, 0.0)
    own_scale = jnp.broadcast_to(jnp.sum(own, axis=1, keepdims=True), (32, 128))
    scale_ref[:32, :] = own_scale
    scale_ref[32:, :] = scales[8:16]
    scale_v = [scales[8:9], scales[9:10]]
    peaks = [None] * 3
    for j in range(LANES):
        score = total[j * 32 : (j + 1) * 32] * own_scale * scale_v[j % 2] * FACTOR
        if j < 2:
            obs_ref[:, j * 128 : (j + 1) * 128] = score
        else:
            p = j // 2 - 1
            peaks[p] = jnp.abs(score) if peaks[p] is None else jnp.maximum(peaks[p], jnp.abs(score))
    out = jnp.zeros((32, 128), F32)
    for p, part in enumerate(peaks):
        out = jnp.where(lane == p, jnp.max(part, axis=1, keepdims=True), out)
    peak_ref[...] = out


def score2_kernel(keep, got, peak1_ref, scale_ref, peak_ref):
    total = keep[...] + got[...]
    own_scale = scale_ref[:32]
    scale_v = [scale_ref[32:33], scale_ref[33:34]]
    lane = lax.broadcasted_iota(jnp.int32, (32, 128), 1)
    peaks = [None] * PERMS
    for j in range(LANES):
        score = jnp.abs(total[j * 32 : (j + 1) * 32] * own_scale * scale_v[(j + LANES) % 2] * FACTOR)
        p = (j + LANES) // 2 - 1
        peaks[p] = score if peaks[p] is None else jnp.maximum(peaks[p], score)
    out = peak1_ref[...]
    for p, part in enumerate(peaks):
        if part is not None:
            best = jnp.max(part, axis=1, keepdims=True)
            out = jnp.where(lane == p, jnp.maximum(out, best), out)
    peak_ref[...] = jnp.transpose(jnp.concatenate([out, jnp.zeros((96, 128), F32)], axis=0))[:8]


def peak_kernel(a, b, c, d, out_ref):
    best = jnp.maximum(jnp.maximum(a[...], b[...]), jnp.maximum(c[...], d[...]))
    out_ref[...] = best[:PERMS, :32]


def scalar_spec(n_in, n_out, grid=(1,)):
    whole = pl.BlockSpec(memory_space=pltpu.VMEM)
    return pltpu.PrefetchScalarGridSpec(
        num_scalar_prefetch=1,
        grid=grid,
        in_specs=[whole] * n_in,
        out_specs=[whole] * n_out,
    )


def in_hbm(value):
    return pltpu.with_memory_space_constraint(value, pltpu.HBM)


def index(axis):
    return jnp.reshape(lax.axis_index(axis), (1,)).astype(jnp.int32)


def program(traits, covariates, genotypes, shuffles):
    core, x, y, zh = index("core"), index("x"), index("y"), index("zh")
    samp = (y * 2 + zh) * 4 + x
    anywhere = pl.BlockSpec(memory_space=pl.ANY)

    pay, xt, dx = call(
        front_kernel,
        [((BLOCKS * C + 40, 128), F32), ((48, ROWS), BF16), ((ROWS, V + 128), BF16)],
        core, in_hbm(traits), in_hbm(covariates.T), in_hbm(genotypes),
        grid_spec=pltpu.PrefetchScalarGridSpec(
            num_scalar_prefetch=1,
            grid=(1,),
            in_specs=[
                pl.BlockSpec((ROWS, HALF), lambda i, c: (0, c[0])),
                pl.BlockSpec((C, ROWS), lambda i, c: (0, 0)),
                pl.BlockSpec((ROWS, V), lambda i, c: (0, 0)),
            ],
            out_specs=[
                pl.BlockSpec((BLOCKS * C + 40, 128), lambda i, c: (0, 0)),
                pl.BlockSpec((48, ROWS), lambda i, c: (0, 0)),
                pl.BlockSpec((ROWS, V + 128), lambda i, c: (0, 0)),
            ],
        ),
        flops=2 * 128 * ROWS * COLS,
        room=14,
    )

    orders = shuffles.reshape(PERMS, 1, ROWS)

    def permuted(first, count, after):
        return call(
            perm_kernel, [((count, ROWS, V + 128), BF16), ((8, 128), F32)],
            samp * ROWS, orders, dx, after,
            grid_spec=pltpu.PrefetchScalarGridSpec(
                num_scalar_prefetch=1,
                grid=(count,),
                in_specs=[
                    pl.BlockSpec((1, 1, ROWS), lambda i, b: (i + first, 0, 0)),
                    pl.BlockSpec((ROWS, V + 128), lambda i, b: (0, 0)),
                    anywhere,
                ],
                out_specs=[
                    pl.BlockSpec((1, ROWS, V + 128), lambda i, b: (i, 0, 0)),
                    pl.BlockSpec((8, 128), lambda i, b: (0, 0)),
                ],
            ),
            flops=2 * count * ROWS * ROWS * (V + 128),
            room=8,
        )

    def summed(value, axis, token):
        parts = [value] + [shift(value, axis, k) for k in (1, 2, 3)]
        return call(sum_kernel, [(value.shape, F32)], *parts, token, room=2)

    turned, at = [], 0
    for axis, count in (("x", SPLIT[0]), ("y", SPLIT[1])):
        rows, token = permuted(at, count, pay)
        pay = summed(pay, axis, token)
        turned.append(rows)
        at += count
    turned.append(permuted(at, SPLIT[2], pay)[0])
    yt = call(
        turn_kernel, [((E, ROWS), BF16)], traits,
        grid_spec=pl.GridSpec(
            grid=(4,),
            in_specs=[pl.BlockSpec((ROWS, 256), lambda i: (0, i))],
            out_specs=pl.BlockSpec((256, ROWS), lambda i: (i, 0)),
        ),
        flops=10**9,
        room=6,
    )
    coef = call(solve_kernel, [((40, V + HALF), F32)], pay, shift(pay, "zh", 1), room=4, flops=10**8)
    far = shift(coef[:, V:], "core", 1)
    g1, g2, ss_v = call(
        geno_kernel,
        [((ROWS, CHUNK), BF16), ((ROWS, CHUNK), BF16), ((8, 128), F32)],
        coef, dx, *turned,
        flops=2 * 128 * ROWS * 2 * CHUNK,
        room=16,
    )
    rt, ss = call(
        resid_kernel,
        [((E, ROWS), BF16), ((SQUARES, 128), F32)],
        core, coef, far, yt, xt, ss_v,
        grid_spec=scalar_spec(5, 2),
        flops=2 * 128 * ROWS * E,
        room=12,
    )

    rt5 = rt.reshape(4, 2, 4, 32, ROWS)
    g_spec = pl.BlockSpec((ROWS, CHUNK), lambda i, t: (0, 0))
    ss_spec = pl.BlockSpec((SQUARES, 128), lambda i, t: (0, 0))

    def cross(axis, k, after):
        onx = axis == "x"
        low = LANES * 128 + (SQUARES if onx else 0)
        return call(
            cross1_kernel if onx else cross2_kernel,
            [((low, 128), F32), ((LANES * 128, 128), F32)],
            ((x if onx else y) + k) % 4,
            *((rt5, g1, ss) if onx else (rt, g2)),
            after,
            grid_spec=pltpu.PrefetchScalarGridSpec(
                num_scalar_prefetch=1,
                grid=(1,),
                in_specs=[
                    *(
                        (pl.BlockSpec((4, 2, 1, 32, ROWS), lambda i, t: (0, 0, t[0], 0, 0)), g_spec, ss_spec)
                        if onx
                        else (pl.BlockSpec((256, ROWS), lambda i, t: (t[0], 0)), g_spec)
                    ),
                    anywhere,
                ],
                out_specs=[
                    pl.BlockSpec((low, 128), lambda i, t: (0, 0)),
                    pl.BlockSpec((LANES * 128, 128), lambda i, t: (0, 0)),
                ],
            ),
            flops=2 * 256 * ROWS * CHUNK,
            room=10,
        )

    part, got = {}, {}
    after = ss
    for k in (2, 3, 1, 0):
        for axis in ("x", "y"):
            part[axis, k] = cross(axis, k, after)
            after = part[axis, k][1]
            low, high = part[axis, k]
            if k == 2:
                got[axis, "low2"] = shift(low, axis, 1)
                got[axis, "high2"] = shift(high, axis, 3)
            elif k == 1:
                got[axis, "high"] = shift(high, axis, 1)
            elif k == 3:
                got[axis, "low"] = shift(low, axis, 3)
    parts = {}
    whole = pl.BlockSpec(memory_space=pltpu.VMEM)
    for axis in ("x", "y"):
        relayed = []
        for k, half, name in ((1, 0, "low2"), (3, 1, "high2")):
            mine = part[axis, k][half]
            relayed.append(
                call(
                    relay_kernel, [(mine.shape, F32)], mine, got[axis, name], after,
                    in_specs=[whole, whole, anywhere], room=2,
                )
            )
        got[axis, "lows"] = shift(relayed[0], axis, 1)
        got[axis, "highs"] = shift(relayed[1], axis, 3)
    keeps = []
    for axis, other, at in (("x", "y", y), ("y", "x", x)):
        rows = LANES * 64 + (SQUARES if axis == "x" else 0)
        low, high = part[axis, 0]
        parts[axis] = call(
            mid_kernel, [((rows, 128), F32)] * 4, at,
            low, got[axis, "low"], got[axis, "lows"], high, got[axis, "high"], got[axis, "highs"],
            grid_spec=scalar_spec(6, 4), flops=10**7, room=4,
        )
        for k in (1, 2, 3):
            parts[axis][k] = shift(parts[axis][k], other, k)
    for axis in ("x", "y"):
        rows = LANES * 32 + (SQUARES if axis == "x" else 0)
        keep, send = call(
            last_kernel, [((rows, 128), F32)] * 2, zh, *parts[axis],
            grid_spec=scalar_spec(4, 2), flops=10**6, room=2,
        )
        keeps.append((keep, shift(send, "zh", 1)))
    observed, peaks, scales = call(
        score1_kernel, [((32, V), F32), ((32, 128), F32), ((40, 128), F32)], samp, *keeps[0],
        grid_spec=scalar_spec(2, 3), flops=10**6, room=4,
    )
    peaks = call(score2_kernel, [((8, 128), F32)], *keeps[1], peaks, scales, flops=10**6, room=4)
    peaks = jnp.maximum(peaks, shift(peaks, "core", 1))
    perm_max = call(
        peak_kernel, [((PERMS, 32), F32)], peaks, *(shift(peaks, "zl", k) for k in (1, 2, 3)),
        room=2,
    )
    return observed, perm_max


def solution(mesh):
    fine = Mesh(mesh.devices.reshape(4, 2, 4, 4, 2), ("y", "zh", "x", "zl", "core"))
    samp, tile = ("y", "zh", "x"), ("zl", "core")
    return jax.shard_map(
        program,
        mesh=fine,
        in_specs=(P(samp, None), P(samp, None), P(samp, tile), P(None, samp)),
        out_specs=(P(samp, tile), P(None, samp)),
        check_vma=False,
    )
```

```python
import math

import jax
import jax.numpy as jnp
from jax import lax
from jax.experimental import pallas as pl
from jax.experimental.pallas import tpu as pltpu
from jax.sharding import Mesh, PartitionSpec as P


C = 32
EPSILON = 1e-05

ROWS = 1024
E = 1024
V = 256
PERMS = 6
HALF = E // 2
COLS = V + HALF + 128
BLOCKS = (V + HALF) // 128
STEP = 256
SPLIT = (3, 2, 1)
SQUARES = 16
CHUNK = (PERMS + 1) * V // 2
LANES = CHUNK // 128
F32 = jnp.float32
BF16 = jnp.bfloat16


def dot(a, b):
    return jnp.dot(a, b, preferred_element_type=F32)


def call(kernel, outs, *args, grid_spec=None, in_specs=None, flops=0, room=4):
    shapes = [jax.ShapeDtypeStruct(s, d) for s, d in outs]
    single = len(shapes) == 1
    extra = {} if grid_spec is None else {"grid_spec": grid_spec}
    if in_specs is not None:
        extra["in_specs"] = in_specs
    nbytes = sum(math.prod(s) * jnp.dtype(d).itemsize for s, d in outs)
    out = pl.pallas_call(
        kernel,
        out_shape=shapes[0] if single else shapes,
        cost_estimate=pl.CostEstimate(flops=flops, bytes_accessed=nbytes, transcendentals=0),
        compiler_params=pltpu.CompilerParams(vmem_limit_bytes=room << 20),
        **extra,
    )(*args)
    return out if single else list(out)


def shifts(axis, k):
    n = lax.axis_size(axis)
    return [(i, (i + k) % n) for i in range(n)]


def shift(value, axis, k):
    return lax.ppermute(value, axis, shifts(axis, k))


def front_kernel(core_ref, traits_hbm, cov_hbm, geno_hbm, pay_ref, xt_ref, dx_ref, traits, cov, geno, sems):
    half = pl.ds(pl.multiple_of(core_ref[0] * HALF, HALF), HALF)
    first = pltpu.make_async_copy(cov_hbm, cov, sems.at[0])
    second = pltpu.make_async_copy(geno_hbm, geno, sems.at[1])
    blocks = []
    for i in range(ROWS // STEP):
        rows = pl.ds(i * STEP, STEP)
        blocks.append(pltpu.make_async_copy(traits_hbm.at[rows, half], traits.at[rows, :], sems.at[2 + i]))
    for copy in (first, second, *blocks):
        copy.start()
    first.wait()
    row = lax.broadcasted_iota(jnp.int32, (128 - C, ROWS), 0)
    tail = jnp.where(row == 0, 1.0, 0.0).astype(F32)
    design_t = jnp.concatenate([cov[...].astype(F32), tail], axis=0)
    design_b = jnp.transpose(design_t).astype(BF16)
    dx_ref[:, V:] = design_b
    xt = design_t[:48].astype(BF16)
    xt_ref[...] = xt
    pay_ref[BLOCKS * C :, :] = dot(xt, design_b)[:40]

    def place(at, part):
        for j in range(part.shape[1] // 128):
            block = part[:, j * 128 : (j + 1) * 128]
            pay_ref[(at + j) * C : (at + j + 1) * C, :] = block[:C]
            ones = BLOCKS * C + C + 1 + at + j
            pay_ref[ones : ones + 1, :] = block[C : C + 1]

    second.wait()
    dosage = geno[...].astype(F32).astype(BF16)
    dx_ref[:, :V] = dosage
    place(0, dot(xt, dosage))
    total = None
    for i, copy in enumerate(blocks):
        copy.wait()
        part = dot(xt[:, i * STEP : (i + 1) * STEP], traits[i * STEP : (i + 1) * STEP, :])
        total = part if total is None else total + part
    place(V // 128, total)


def turn_kernel(traits_ref, out_ref):
    out_ref[...] = jnp.transpose(traits_ref[...])


def perm_kernel(base_ref, order_ref, dx_ref, after_ref, out_ref, token_ref):
    del after_ref
    order = order_ref[0] - base_ref[0]
    for at in range(0, ROWS, 256):
        row = lax.broadcasted_iota(jnp.int32, (256, ROWS), 0) + at
        pick = jnp.where(row == order, 1.0, 0.0).astype(BF16)
        out_ref[0, at : at + 256, :] = dot(pick, dx_ref[...]).astype(BF16)
    token_ref[...] = jnp.zeros(token_ref.shape, F32)


def sum_kernel(a, b, c, d, token, out):
    del token
    out[...] = (a[...] + c[...]) + (b[...] + d[...])


def solve_kernel(own_ref, far_ref, out_ref):
    total = own_ref[...] + far_ref[...]
    base = BLOCKS * C
    m = [
        [total[j * C + g * 8 : j * C + g * 8 + 8] for j in range(BLOCKS)] + [total[base + g * 8 : base + g * 8 + 8]]
        for g in range(C // 8)
    ]
    wide = (8, 128)
    zero = jnp.broadcast_to(total[base + 39 : base + 40], wide)
    ones = [total[base + C + 1 + j : base + C + 2 + j] for j in range(BLOCKS)] + [total[base + C : base + C + 1]]
    m.append([jnp.broadcast_to(part, wide) for part in ones])
    row_id = lax.broadcasted_iota(jnp.int32, wide, 0)

    def line_of(part, line):
        return jnp.broadcast_to(part[line : line + 1], wide)

    ones = [jnp.broadcast_to(part[BLOCKS][:, C : C + 1], wide) + zero for part in m]
    inverse = 1.0 / line_of(ones[-1], 0)
    for j in range(BLOCKS + 1):
        row = line_of(m[-1][j], 0) * inverse
        for g in range(len(m)):
            m[g][j] = m[g][j] - ones[g] * row if g < C // 8 else row
    for k in range(0, C, 2):
        here, line = k // 8, k % 8
        left = [jnp.broadcast_to(part[BLOCKS][:, k : k + 1], wide) + zero for part in m]
        right = [jnp.broadcast_to(part[BLOCKS][:, k + 1 : k + 2], wide) + zero for part in m]
        p, q = line_of(left[here], line), line_of(right[here], line)
        r, s = line_of(left[here], line + 1), line_of(right[here], line + 1)
        inverse = 1.0 / (p * s - q * r)
        p, q, r, s = p * inverse, q * inverse, r * inverse, s * inverse
        for j in range(BLOCKS + 1):
            top, low = line_of(m[here][j], line), line_of(m[here][j], line + 1)
            top, low = s * top - q * low, p * low - r * top
            for g in range(len(m)):
                rest = m[g][j] - left[g] * top - right[g] * low
                if g == here:
                    rest = jnp.where(row_id == line, top, jnp.where(row_id == line + 1, low, rest))
                m[g][j] = rest
    for g in range(len(m)):
        for j in range(BLOCKS):
            done = m[g][j] if g < C // 8 else jnp.where(row_id == 0, m[g][j], 0.0)
            out_ref[g * 8 : g * 8 + 8, j * 128 : (j + 1) * 128] = done


def geno_kernel(own_ref, dx_ref, dxp1_ref, dxp2_ref, dxp3_ref, g1_ref, g2_ref, ss_ref):
    gamma = jnp.concatenate([own_ref[:, :V], jnp.zeros((88, V), F32)], axis=0).astype(BF16)
    res_g = dx_ref[:, :V].astype(F32) - dot(dx_ref[:, V:], gamma)
    g1_ref[:, :V] = res_g.astype(BF16)
    ss_v = jnp.sum(res_g * res_g, axis=0, keepdims=True)
    ss_ref[...] = jnp.concatenate([ss_v[:, :128], ss_v[:, 128:], jnp.zeros((6, 128), F32)], axis=0)
    places = [(ref, q) for ref in (dxp1_ref, dxp2_ref, dxp3_ref) for q in range(ref.shape[0])]
    for p, (src, q) in enumerate(places):
        g = (src[q, :, :V].astype(F32) - dot(src[q, :, V:], gamma)).astype(BF16)
        at = (p + 1) * V
        if at + V <= CHUNK:
            g1_ref[:, at : at + V] = g
        elif at >= CHUNK:
            g2_ref[:, at - CHUNK : at - CHUNK + V] = g
        else:
            g1_ref[:, at:] = g[:, : CHUNK - at]
            g2_ref[:, : at + V - CHUNK] = g[:, CHUNK - at :]


def resid_kernel(core_ref, own_ref, far_ref, yt_ref, xt_ref, ss_v_ref, rt_ref, ss_ref):
    core = core_ref[0]
    xt = xt_ref[...]
    mine = own_ref[:, V:]
    other = far_ref[...]
    first = jnp.where(core == 0, mine, other)
    second = jnp.where(core == 0, other, mine)
    coef = jnp.concatenate([jnp.concatenate([first, second], axis=1), jnp.zeros((8, E), F32)], axis=0)
    coef_t = jnp.transpose(coef).astype(BF16)
    for j in range(E // 128):
        at = j * 128
        res = yt_ref[at : at + 128, :].astype(F32) - dot(coef_t[at : at + 128], xt)
        rt_ref[at : at + 128, :] = res.astype(BF16)
        sq = res * res
        lanes = sq[:, :128]
        for b in range(128, ROWS, 128):
            lanes = lanes + sq[:, b : b + 128]
        ss_ref[j : j + 1, :] = jnp.sum(jnp.transpose(lanes), axis=0, keepdims=True)
    ss_ref[8:, :] = ss_v_ref[...]


def lanes_to_rows(out_ref, value):
    rows = value.shape[0]
    for j in range(LANES):
        out_ref[j * rows : (j + 1) * rows, :] = value[:, j * 128 : (j + 1) * 128]


def cross1_kernel(to_ref, rt_ref, g_ref, ss_ref, after_ref, low_ref, high_ref):
    del to_ref, after_ref
    lanes_to_rows(low_ref, dot(rt_ref[:, 0, 0].reshape(128, ROWS), g_ref[...]))
    low_ref[LANES * 128 :, :] = ss_ref[...]
    lanes_to_rows(high_ref, dot(rt_ref[:, 1, 0].reshape(128, ROWS), g_ref[...]))


def cross2_kernel(to_ref, rt_ref, g_ref, after_ref, low_ref, high_ref):
    del to_ref, after_ref
    lanes_to_rows(low_ref, dot(rt_ref[:128], g_ref[...]))
    lanes_to_rows(high_ref, dot(rt_ref[128:], g_ref[...]))


def relay_kernel(a, b, after, out):
    del after
    out[...] = a[...] + b[...]


def mid_kernel(at_ref, low, low_near, low_far, high, high_near, high_far, *outs):
    me = at_ref[0]
    for k in range(4):
        for j in range(LANES):
            rows = pl.ds(pl.multiple_of(j * 128 + ((me + k) % 4) * 32, 32), 32)
            outs[k][j * 64 : j * 64 + 32, :] = low[rows, :] + (low_near[rows, :] + low_far[rows, :])
            outs[k][j * 64 + 32 : j * 64 + 64, :] = high[rows, :] + (high_near[rows, :] + high_far[rows, :])
        if outs[k].shape[0] > LANES * 64:
            rows = pl.ds(LANES * 128, SQUARES)
            outs[k][LANES * 64 :, :] = low[rows, :] + (low_near[rows, :] + low_far[rows, :])


def last_kernel(at_ref, a, b, c, d, keep, send):
    z = at_ref[0]
    for out, half in ((keep, z), (send, 1 - z)):
        for j in range(LANES):
            rows = pl.ds(pl.multiple_of(j * 64 + half * 32, 32), 32)
            out[j * 32 : (j + 1) * 32, :] = (a[rows, :] + c[rows, :]) + (b[rows, :] + d[rows, :])
        if out.shape[0] > LANES * 32:
            rows = pl.ds(LANES * 64, SQUARES)
            out[LANES * 32 :, :] = (a[rows, :] + c[rows, :]) + (b[rows, :] + d[rows, :])


FACTOR = math.sqrt(32 * ROWS - C - 2) / (32 * ROWS)


def score1_kernel(at_ref, keep, got, obs_ref, peak_ref, scale_ref):
    total = keep[...] + got[...]
    scales = lax.rsqrt(total[LANES * 32 :] / (32 * ROWS) + EPSILON)
    place = lax.broadcasted_iota(jnp.int32, (SQUARES, 128), 0)
    lane = lax.broadcasted_iota(jnp.int32, (32, 128), 1)
    row = lax.broadcasted_iota(jnp.int32, (32, 128), 0)
    scale_e = jnp.sum(jnp.where(place == at_ref[0] // 4, scales, 0.0), axis=0, keepdims=True)
    own = jnp.where(lane == row + (at_ref[0] % 4) * 32, scale_e, 0.0)
    own_scale = jnp.broadcast_to(jnp.sum(own, axis=1, keepdims=True), (32, 128))
    scale_ref[:32, :] = own_scale
    scale_ref[32:, :] = scales[8:16]
    scale_v = [scales[8:9], scales[9:10]]
    peaks = [None] * 3
    for j in range(LANES):
        score = total[j * 32 : (j + 1) * 32] * own_scale * scale_v[j % 2] * FACTOR
        if j < 2:
            obs_ref[:, j * 128 : (j + 1) * 128] = score
        else:
            p = j // 2 - 1
            peaks[p] = jnp.abs(score) if peaks[p] is None else jnp.maximum(peaks[p], jnp.abs(score))
    out = jnp.zeros((32, 128), F32)
    for p, part in enumerate(peaks):
        out = jnp.where(lane == p, jnp.max(part, axis=1, keepdims=True), out)
    peak_ref[...] = out


def score2_kernel(keep, got, peak1_ref, scale_ref, peak_ref):
    total = keep[...] + got[...]
    own_scale = scale_ref[:32]
    scale_v = [scale_ref[32:33], scale_ref[33:34]]
    lane = lax.broadcasted_iota(jnp.int32, (32, 128), 1)
    peaks = [None] * PERMS
    for j in range(LANES):
        score = jnp.abs(total[j * 32 : (j + 1) * 32] * own_scale * scale_v[(j + LANES) % 2] * FACTOR)
        p = (j + LANES) // 2 - 1
        peaks[p] = score if peaks[p] is None else jnp.maximum(peaks[p], score)
    out = peak1_ref[...]
    for p, part in enumerate(peaks):
        if part is not None:
            best = jnp.max(part, axis=1, keepdims=True)
            out = jnp.where(lane == p, jnp.maximum(out, best), out)
    peak_ref[...] = jnp.transpose(jnp.concatenate([out, jnp.zeros((96, 128), F32)], axis=0))[:8]


def peak_kernel(a, b, c, d, out_ref):
    best = jnp.maximum(jnp.maximum(a[...], b[...]), jnp.maximum(c[...], d[...]))
    out_ref[...] = best[:PERMS, :32]


def scalar_spec(n_in, n_out, grid=(1,)):
    whole = pl.BlockSpec(memory_space=pltpu.VMEM)
    return pltpu.PrefetchScalarGridSpec(
        num_scalar_prefetch=1,
        grid=grid,
        in_specs=[whole] * n_in,
        out_specs=[whole] * n_out,
    )


def in_hbm(value):
    return pltpu.with_memory_space_constraint(value, pltpu.HBM)


def index(axis):
    return jnp.reshape(lax.axis_index(axis), (1,)).astype(jnp.int32)


def program(traits, covariates, genotypes, shuffles):
    core, x, y, zh = index("core"), index("x"), index("y"), index("zh")
    samp = (y * 2 + zh) * 4 + x
    anywhere = pl.BlockSpec(memory_space=pl.ANY)

    pay, xt, dx = call(
        front_kernel,
        [((BLOCKS * C + 40, 128), F32), ((48, ROWS), BF16), ((ROWS, V + 128), BF16)],
        core, in_hbm(traits), in_hbm(covariates.T), in_hbm(genotypes),
        grid_spec=pltpu.PrefetchScalarGridSpec(
            num_scalar_prefetch=1,
            grid=(1,),
            in_specs=[anywhere] * 3,
            out_specs=[pl.BlockSpec(memory_space=pltpu.VMEM)] * 3,
            scratch_shapes=[
                pltpu.VMEM((ROWS, HALF), BF16),
                pltpu.VMEM((C, ROWS), BF16),
                pltpu.VMEM((ROWS, V), jnp.int32),
                pltpu.SemaphoreType.DMA((2 + ROWS // STEP,)),
            ],
        ),
        flops=2 * 128 * ROWS * COLS,
        room=14,
    )

    orders = shuffles.reshape(PERMS, 1, ROWS)

    def permuted(first, count, after):
        return call(
            perm_kernel, [((count, ROWS, V + 128), BF16), ((8, 128), F32)],
            samp * ROWS, orders, dx, after,
            grid_spec=pltpu.PrefetchScalarGridSpec(
                num_scalar_prefetch=1,
                grid=(count,),
                in_specs=[
                    pl.BlockSpec((1, 1, ROWS), lambda i, b: (i + first, 0, 0)),
                    pl.BlockSpec((ROWS, V + 128), lambda i, b: (0, 0)),
                    anywhere,
                ],
                out_specs=[
                    pl.BlockSpec((1, ROWS, V + 128), lambda i, b: (i, 0, 0)),
                    pl.BlockSpec((8, 128), lambda i, b: (0, 0)),
                ],
            ),
            flops=2 * count * ROWS * ROWS * (V + 128),
            room=8,
        )

    def summed(value, axis, token):
        parts = [value] + [shift(value, axis, k) for k in (1, 2, 3)]
        return call(sum_kernel, [(value.shape, F32)], *parts, token, room=2)

    turned, at = [], 0
    for axis, count in (("x", SPLIT[0]), ("y", SPLIT[1])):
        rows, token = permuted(at, count, pay)
        pay = summed(pay, axis, token)
        turned.append(rows)
        at += count
    turned.append(permuted(at, SPLIT[2], pay)[0])
    yt = call(
        turn_kernel, [((E, ROWS), BF16)], traits,
        grid_spec=pl.GridSpec(
            grid=(4,),
            in_specs=[pl.BlockSpec((ROWS, 256), lambda i: (0, i))],
            out_specs=pl.BlockSpec((256, ROWS), lambda i: (i, 0)),
        ),
        flops=10**9,
        room=6,
    )
    coef = call(solve_kernel, [((40, V + HALF), F32)], pay, shift(pay, "zh", 1), room=4, flops=10**8)
    far = shift(coef[:, V:], "core", 1)
    g1, g2, ss_v = call(
        geno_kernel,
        [((ROWS, CHUNK), BF16), ((ROWS, CHUNK), BF16), ((8, 128), F32)],
        coef, dx, *turned,
        flops=2 * 128 * ROWS * 2 * CHUNK,
        room=16,
    )
    rt, ss = call(
        resid_kernel,
        [((E, ROWS), BF16), ((SQUARES, 128), F32)],
        core, coef, far, yt, xt, ss_v,
        grid_spec=scalar_spec(5, 2),
        flops=2 * 128 * ROWS * E,
        room=12,
    )

    rt5 = rt.reshape(4, 2, 4, 32, ROWS)
    g_spec = pl.BlockSpec((ROWS, CHUNK), lambda i, t: (0, 0))
    ss_spec = pl.BlockSpec((SQUARES, 128), lambda i, t: (0, 0))

    def cross(axis, k, after):
        onx = axis == "x"
        low = LANES * 128 + (SQUARES if onx else 0)
        return call(
            cross1_kernel if onx else cross2_kernel,
            [((low, 128), F32), ((LANES * 128, 128), F32)],
            ((x if onx else y) + k) % 4,
            *((rt5, g1, ss) if onx else (rt, g2)),
            after,
            grid_spec=pltpu.PrefetchScalarGridSpec(
                num_scalar_prefetch=1,
                grid=(1,),
                in_specs=[
                    *(
                        (pl.BlockSpec((4, 2, 1, 32, ROWS), lambda i, t: (0, 0, t[0], 0, 0)), g_spec, ss_spec)
                        if onx
                        else (pl.BlockSpec((256, ROWS), lambda i, t: (t[0], 0)), g_spec)
                    ),
                    anywhere,
                ],
                out_specs=[
                    pl.BlockSpec((low, 128), lambda i, t: (0, 0)),
                    pl.BlockSpec((LANES * 128, 128), lambda i, t: (0, 0)),
                ],
            ),
            flops=2 * 256 * ROWS * CHUNK,
            room=10,
        )

    part, got = {}, {}
    after = ss
    for k in (2, 3, 1, 0):
        for axis in ("x", "y"):
            part[axis, k] = cross(axis, k, after)
            after = part[axis, k][1]
            low, high = part[axis, k]
            if k == 2:
                got[axis, "low2"] = shift(low, axis, 1)
                got[axis, "high2"] = shift(high, axis, 3)
            elif k == 1:
                got[axis, "high"] = shift(high, axis, 1)
            elif k == 3:
                got[axis, "low"] = shift(low, axis, 3)
    parts = {}
    whole = pl.BlockSpec(memory_space=pltpu.VMEM)
    for axis in ("x", "y"):
        relayed = []
        for k, half, name in ((1, 0, "low2"), (3, 1, "high2")):
            mine = part[axis, k][half]
            relayed.append(
                call(
                    relay_kernel, [(mine.shape, F32)], mine, got[axis, name], after,
                    in_specs=[whole, whole, anywhere], room=2,
                )
            )
        got[axis, "lows"] = shift(relayed[0], axis, 1)
        got[axis, "highs"] = shift(relayed[1], axis, 3)
    keeps = []
    for axis, other, at in (("x", "y", y), ("y", "x", x)):
        rows = LANES * 64 + (SQUARES if axis == "x" else 0)
        low, high = part[axis, 0]
        parts[axis] = call(
            mid_kernel, [((rows, 128), F32)] * 4, at,
            low, got[axis, "low"], got[axis, "lows"], high, got[axis, "high"], got[axis, "highs"],
            grid_spec=scalar_spec(6, 4), flops=10**7, room=4,
        )
        for k in (1, 2, 3):
            parts[axis][k] = shift(parts[axis][k], other, k)
    for axis in ("x", "y"):
        rows = LANES * 32 + (SQUARES if axis == "x" else 0)
        keep, send = call(
            last_kernel, [((rows, 128), F32)] * 2, zh, *parts[axis],
            grid_spec=scalar_spec(4, 2), flops=10**6, room=2,
        )
        keeps.append((keep, shift(send, "zh", 1)))
    observed, peaks, scales = call(
        score1_kernel, [((32, V), F32), ((32, 128), F32), ((40, 128), F32)], samp, *keeps[0],
        grid_spec=scalar_spec(2, 3), flops=10**6, room=4,
    )
    peaks = call(score2_kernel, [((8, 128), F32)], *keeps[1], peaks, scales, flops=10**6, room=4)
    peaks = jnp.maximum(peaks, shift(peaks, "core", 1))
    perm_max = call(
        peak_kernel, [((PERMS, 32), F32)], peaks, *(shift(peaks, "zl", k) for k in (1, 2, 3)),
        room=2,
    )
    return observed, perm_max


def solution(mesh):
    fine = Mesh(mesh.devices.reshape(4, 2, 4, 4, 2), ("y", "zh", "x", "zl", "core"))
    samp, tile = ("y", "zh", "x"), ("zl", "core")
    return jax.shard_map(
        program,
        mesh=fine,
        in_specs=(P(samp, None), P(samp, None), P(samp, tile), P(None, samp)),
        out_specs=(P(samp, tile), P(None, samp)),
        check_vma=False,
    )
```

```python
import math

import jax
import jax.numpy as jnp
from jax import lax
from jax.experimental import pallas as pl
from jax.experimental.pallas import tpu as pltpu
from jax.sharding import Mesh, PartitionSpec as P


C = 32
EPSILON = 1e-05

ROWS = 1024
E = 1024
V = 256
PERMS = 6
HALF = E // 2
COLS = V + HALF + 128
BLOCKS = (V + HALF) // 128
STEP = 256
SPLIT = (3, 2, 1)
SQUARES = 16
CHUNK = (PERMS + 1) * V // 2
LANES = CHUNK // 128
F32 = jnp.float32
BF16 = jnp.bfloat16


def dot(a, b):
    return jnp.dot(a, b, preferred_element_type=F32)


def call(kernel, outs, *args, grid_spec=None, in_specs=None, flops=0, room=4):
    shapes = [jax.ShapeDtypeStruct(s, d) for s, d in outs]
    single = len(shapes) == 1
    extra = {} if grid_spec is None else {"grid_spec": grid_spec}
    if in_specs is not None:
        extra["in_specs"] = in_specs
    nbytes = sum(math.prod(s) * jnp.dtype(d).itemsize for s, d in outs)
    out = pl.pallas_call(
        kernel,
        out_shape=shapes[0] if single else shapes,
        cost_estimate=pl.CostEstimate(flops=flops, bytes_accessed=nbytes, transcendentals=0),
        compiler_params=pltpu.CompilerParams(vmem_limit_bytes=room << 20),
        **extra,
    )(*args)
    return out if single else list(out)


def shifts(axis, k):
    n = lax.axis_size(axis)
    return [(i, (i + k) % n) for i in range(n)]


def shift(value, axis, k):
    return lax.ppermute(value, axis, shifts(axis, k))


def front_kernel(core_ref, traits_hbm, cov_hbm, geno_hbm, pay_ref, xt_ref, dx_ref, traits, cov, geno, sems):
    half = pl.ds(pl.multiple_of(core_ref[0] * HALF, HALF), HALF)
    first = pltpu.make_async_copy(cov_hbm, cov, sems.at[0])
    dosages, blocks = [], []
    for i in range(ROWS // STEP):
        rows = pl.ds(i * STEP, STEP)
        dosages.append(pltpu.make_async_copy(geno_hbm.at[rows, :], geno.at[rows, :], sems.at[1 + i]))
        blocks.append(pltpu.make_async_copy(traits_hbm.at[rows, half], traits.at[rows, :], sems.at[1 + ROWS // STEP + i]))
    for copy in (first, *dosages, *blocks):
        copy.start()
    first.wait()
    row = lax.broadcasted_iota(jnp.int32, (128 - C, ROWS), 0)
    tail = jnp.where(row == 0, 1.0, 0.0).astype(F32)
    design_t = jnp.concatenate([cov[...].astype(F32), tail], axis=0)
    design_b = jnp.transpose(design_t).astype(BF16)
    dx_ref[:, V:] = design_b
    xt = design_t[:48].astype(BF16)
    xt_ref[...] = xt
    pay_ref[BLOCKS * C :, :] = dot(xt, design_b)[:40]

    def place(at, part):
        for j in range(part.shape[1] // 128):
            block = part[:, j * 128 : (j + 1) * 128]
            pay_ref[(at + j) * C : (at + j + 1) * C, :] = block[:C]
            ones = BLOCKS * C + C + 1 + at + j
            pay_ref[ones : ones + 1, :] = block[C : C + 1]

    for copy in dosages:
        copy.wait()
    dosage = geno[...].astype(F32).astype(BF16)
    dx_ref[:, :V] = dosage
    place(0, dot(xt, dosage))
    total = None
    for i, copy in enumerate(blocks):
        copy.wait()
        part = dot(xt[:, i * STEP : (i + 1) * STEP], traits[i * STEP : (i + 1) * STEP, :])
        total = part if total is None else total + part
    place(V // 128, total)


def turn_kernel(traits_ref, out_ref):
    out_ref[...] = jnp.transpose(traits_ref[...])


def perm_kernel(base_ref, order_ref, dx_ref, after_ref, out_ref, token_ref):
    del after_ref
    order = order_ref[0] - base_ref[0]
    for at in range(0, ROWS, 256):
        row = lax.broadcasted_iota(jnp.int32, (256, ROWS), 0) + at
        pick = jnp.where(row == order, 1.0, 0.0).astype(BF16)
        out_ref[0, at : at + 256, :] = dot(pick, dx_ref[...]).astype(BF16)
    token_ref[...] = jnp.zeros(token_ref.shape, F32)


def sum_kernel(a, b, c, d, token, out):
    del token
    out[...] = (a[...] + c[...]) + (b[...] + d[...])


def solve_kernel(own_ref, far_ref, out_ref):
    total = own_ref[...] + far_ref[...]
    base = BLOCKS * C
    m = [
        [total[j * C + g * 8 : j * C + g * 8 + 8] for j in range(BLOCKS)] + [total[base + g * 8 : base + g * 8 + 8]]
        for g in range(C // 8)
    ]
    wide = (8, 128)
    zero = jnp.broadcast_to(total[base + 39 : base + 40], wide)
    ones = [total[base + C + 1 + j : base + C + 2 + j] for j in range(BLOCKS)] + [total[base + C : base + C + 1]]
    m.append([jnp.broadcast_to(part, wide) for part in ones])
    row_id = lax.broadcasted_iota(jnp.int32, wide, 0)

    def line_of(part, line):
        return jnp.broadcast_to(part[line : line + 1], wide)

    ones = [jnp.broadcast_to(part[BLOCKS][:, C : C + 1], wide) + zero for part in m]
    inverse = 1.0 / line_of(ones[-1], 0)
    for j in range(BLOCKS + 1):
        row = line_of(m[-1][j], 0) * inverse
        for g in range(len(m)):
            m[g][j] = m[g][j] - ones[g] * row if g < C // 8 else row
    for k in range(0, C, 2):
        here, line = k // 8, k % 8
        left = [jnp.broadcast_to(part[BLOCKS][:, k : k + 1], wide) + zero for part in m]
        right = [jnp.broadcast_to(part[BLOCKS][:, k + 1 : k + 2], wide) + zero for part in m]
        p, q = line_of(left[here], line), line_of(right[here], line)
        r, s = line_of(left[here], line + 1), line_of(right[here], line + 1)
        inverse = 1.0 / (p * s - q * r)
        p, q, r, s = p * inverse, q * inverse, r * inverse, s * inverse
        for j in range(BLOCKS + 1):
            top, low = line_of(m[here][j], line), line_of(m[here][j], line + 1)
            top, low = s * top - q * low, p * low - r * top
            for g in range(len(m)):
                rest = m[g][j] - left[g] * top - right[g] * low
                if g == here:
                    rest = jnp.where(row_id == line, top, jnp.where(row_id == line + 1, low, rest))
                m[g][j] = rest
    for g in range(len(m)):
        for j in range(BLOCKS):
            done = m[g][j] if g < C // 8 else jnp.where(row_id == 0, m[g][j], 0.0)
            out_ref[g * 8 : g * 8 + 8, j * 128 : (j + 1) * 128] = done


def geno_kernel(own_ref, dx_ref, dxp1_ref, dxp2_ref, dxp3_ref, g1_ref, g2_ref, ss_ref):
    gamma = jnp.concatenate([own_ref[:, :V], jnp.zeros((88, V), F32)], axis=0).astype(BF16)
    res_g = dx_ref[:, :V].astype(F32) - dot(dx_ref[:, V:], gamma)
    g1_ref[:, :V] = res_g.astype(BF16)
    ss_v = jnp.sum(res_g * res_g, axis=0, keepdims=True)
    ss_ref[...] = jnp.concatenate([ss_v[:, :128], ss_v[:, 128:], jnp.zeros((6, 128), F32)], axis=0)
    places = [(ref, q) for ref in (dxp1_ref, dxp2_ref, dxp3_ref) for q in range(ref.shape[0])]
    for p, (src, q) in enumerate(places):
        g = (src[q, :, :V].astype(F32) - dot(src[q, :, V:], gamma)).astype(BF16)
        at = (p + 1) * V
        if at + V <= CHUNK:
            g1_ref[:, at : at + V] = g
        elif at >= CHUNK:
            g2_ref[:, at - CHUNK : at - CHUNK + V] = g
        else:
            g1_ref[:, at:] = g[:, : CHUNK - at]
            g2_ref[:, : at + V - CHUNK] = g[:, CHUNK - at :]


def resid_kernel(core_ref, own_ref, far_ref, yt_ref, xt_ref, ss_v_ref, rt_ref, ss_ref):
    core = core_ref[0]
    xt = xt_ref[...]
    mine = own_ref[:, V:]
    other = far_ref[...]
    first = jnp.where(core == 0, mine, other)
    second = jnp.where(core == 0, other, mine)
    coef = jnp.concatenate([jnp.concatenate([first, second], axis=1), jnp.zeros((8, E), F32)], axis=0)
    coef_t = jnp.transpose(coef).astype(BF16)
    for j in range(E // 128):
        at = j * 128
        res = yt_ref[at : at + 128, :].astype(F32) - dot(coef_t[at : at + 128], xt)
        rt_ref[at : at + 128, :] = res.astype(BF16)
        sq = res * res
        lanes = sq[:, :128]
        for b in range(128, ROWS, 128):
            lanes = lanes + sq[:, b : b + 128]
        ss_ref[j : j + 1, :] = jnp.sum(jnp.transpose(lanes), axis=0, keepdims=True)
    ss_ref[8:, :] = ss_v_ref[...]


def lanes_to_rows(out_ref, value):
    rows = value.shape[0]
    for j in range(LANES):
        out_ref[j * rows : (j + 1) * rows, :] = value[:, j * 128 : (j + 1) * 128]


def cross1_kernel(to_ref, rt_ref, g_ref, ss_ref, after_ref, low_ref, high_ref):
    del to_ref, after_ref
    lanes_to_rows(low_ref, dot(rt_ref[:, 0, 0].reshape(128, ROWS), g_ref[...]))
    low_ref[LANES * 128 :, :] = ss_ref[...]
    lanes_to_rows(high_ref, dot(rt_ref[:, 1, 0].reshape(128, ROWS), g_ref[...]))


def cross2_kernel(to_ref, rt_ref, g_ref, after_ref, low_ref, high_ref):
    del to_ref, after_ref
    lanes_to_rows(low_ref, dot(rt_ref[:128], g_ref[...]))
    lanes_to_rows(high_ref, dot(rt_ref[128:], g_ref[...]))


def relay_kernel(a, b, after, out):
    del after
    out[...] = a[...] + b[...]


def mid_kernel(at_ref, low, low_near, low_far, high, high_near, high_far, *outs):
    me = at_ref[0]
    for k in range(4):
        for j in range(LANES):
            rows = pl.ds(pl.multiple_of(j * 128 + ((me + k) % 4) * 32, 32), 32)
            outs[k][j * 64 : j * 64 + 32, :] = low[rows, :] + (low_near[rows, :] + low_far[rows, :])
            outs[k][j * 64 + 32 : j * 64 + 64, :] = high[rows, :] + (high_near[rows, :] + high_far[rows, :])
        if outs[k].shape[0] > LANES * 64:
            rows = pl.ds(LANES * 128, SQUARES)
            outs[k][LANES * 64 :, :] = low[rows, :] + (low_near[rows, :] + low_far[rows, :])


def last_kernel(at_ref, a, b, c, d, keep, send):
    z = at_ref[0]
    for out, half in ((keep, z), (send, 1 - z)):
        for j in range(LANES):
            rows = pl.ds(pl.multiple_of(j * 64 + half * 32, 32), 32)
            out[j * 32 : (j + 1) * 32, :] = (a[rows, :] + c[rows, :]) + (b[rows, :] + d[rows, :])
        if out.shape[0] > LANES * 32:
            rows = pl.ds(LANES * 64, SQUARES)
            out[LANES * 32 :, :] = (a[rows, :] + c[rows, :]) + (b[rows, :] + d[rows, :])


FACTOR = math.sqrt(32 * ROWS - C - 2) / (32 * ROWS)


def score1_kernel(at_ref, keep, got, obs_ref, peak_ref, scale_ref):
    total = keep[...] + got[...]
    scales = lax.rsqrt(total[LANES * 32 :] / (32 * ROWS) + EPSILON)
    place = lax.broadcasted_iota(jnp.int32, (SQUARES, 128), 0)
    lane = lax.broadcasted_iota(jnp.int32, (32, 128), 1)
    row = lax.broadcasted_iota(jnp.int32, (32, 128), 0)
    scale_e = jnp.sum(jnp.where(place == at_ref[0] // 4, scales, 0.0), axis=0, keepdims=True)
    own = jnp.where(lane == row + (at_ref[0] % 4) * 32, scale_e, 0.0)
    own_scale = jnp.broadcast_to(jnp.sum(own, axis=1, keepdims=True), (32, 128))
    scale_ref[:32, :] = own_scale
    scale_ref[32:, :] = scales[8:16]
    scale_v = [scales[8:9], scales[9:10]]
    peaks = [None] * 3
    for j in range(LANES):
        score = total[j * 32 : (j + 1) * 32] * own_scale * scale_v[j % 2] * FACTOR
        if j < 2:
            obs_ref[:, j * 128 : (j + 1) * 128] = score
        else:
            p = j // 2 - 1
            peaks[p] = jnp.abs(score) if peaks[p] is None else jnp.maximum(peaks[p], jnp.abs(score))
    out = jnp.zeros((32, 128), F32)
    for p, part in enumerate(peaks):
        out = jnp.where(lane == p, jnp.max(part, axis=1, keepdims=True), out)
    peak_ref[...] = out


def score2_kernel(keep, got, peak1_ref, scale_ref, peak_ref):
    total = keep[...] + got[...]
    own_scale = scale_ref[:32]
    scale_v = [scale_ref[32:33], scale_ref[33:34]]
    lane = lax.broadcasted_iota(jnp.int32, (32, 128), 1)
    peaks = [None] * PERMS
    for j in range(LANES):
        score = jnp.abs(total[j * 32 : (j + 1) * 32] * own_scale * scale_v[(j + LANES) % 2] * FACTOR)
        p = (j + LANES) // 2 - 1
        peaks[p] = score if peaks[p] is None else jnp.maximum(peaks[p], score)
    out = peak1_ref[...]
    for p, part in enumerate(peaks):
        if part is not None:
            best = jnp.max(part, axis=1, keepdims=True)
            out = jnp.where(lane == p, jnp.maximum(out, best), out)
    peak_ref[...] = jnp.transpose(jnp.concatenate([out, jnp.zeros((96, 128), F32)], axis=0))[:8]


def peak_kernel(a, b, c, d, out_ref):
    best = jnp.maximum(jnp.maximum(a[...], b[...]), jnp.maximum(c[...], d[...]))
    out_ref[...] = best[:PERMS, :32]


def scalar_spec(n_in, n_out, grid=(1,)):
    whole = pl.BlockSpec(memory_space=pltpu.VMEM)
    return pltpu.PrefetchScalarGridSpec(
        num_scalar_prefetch=1,
        grid=grid,
        in_specs=[whole] * n_in,
        out_specs=[whole] * n_out,
    )


def in_hbm(value):
    return pltpu.with_memory_space_constraint(value, pltpu.HBM)


def index(axis):
    return jnp.reshape(lax.axis_index(axis), (1,)).astype(jnp.int32)


def program(traits, covariates, genotypes, shuffles):
    core, x, y, zh = index("core"), index("x"), index("y"), index("zh")
    samp = (y * 2 + zh) * 4 + x
    anywhere = pl.BlockSpec(memory_space=pl.ANY)

    pay, xt, dx = call(
        front_kernel,
        [((BLOCKS * C + 40, 128), F32), ((48, ROWS), BF16), ((ROWS, V + 128), BF16)],
        core, in_hbm(traits), in_hbm(covariates.T), in_hbm(genotypes),
        grid_spec=pltpu.PrefetchScalarGridSpec(
            num_scalar_prefetch=1,
            grid=(1,),
            in_specs=[anywhere] * 3,
            out_specs=[pl.BlockSpec(memory_space=pltpu.VMEM)] * 3,
            scratch_shapes=[
                pltpu.VMEM((ROWS, HALF), BF16),
                pltpu.VMEM((C, ROWS), BF16),
                pltpu.VMEM((ROWS, V), jnp.int32),
                pltpu.SemaphoreType.DMA((1 + 2 * (ROWS // STEP),)),
            ],
        ),
        flops=2 * 128 * ROWS * COLS,
        room=14,
    )

    orders = shuffles.reshape(PERMS, 1, ROWS)

    def permuted(first, count, after):
        return call(
            perm_kernel, [((count, ROWS, V + 128), BF16), ((8, 128), F32)],
            samp * ROWS, orders, dx, after,
            grid_spec=pltpu.PrefetchScalarGridSpec(
                num_scalar_prefetch=1,
                grid=(count,),
                in_specs=[
                    pl.BlockSpec((1, 1, ROWS), lambda i, b: (i + first, 0, 0)),
                    pl.BlockSpec((ROWS, V + 128), lambda i, b: (0, 0)),
                    anywhere,
                ],
                out_specs=[
                    pl.BlockSpec((1, ROWS, V + 128), lambda i, b: (i, 0, 0)),
                    pl.BlockSpec((8, 128), lambda i, b: (0, 0)),
                ],
            ),
            flops=2 * count * ROWS * ROWS * (V + 128),
            room=8,
        )

    def summed(value, axis, token):
        parts = [value] + [shift(value, axis, k) for k in (1, 2, 3)]
        return call(sum_kernel, [(value.shape, F32)], *parts, token, room=2)

    turned, at = [], 0
    for axis, count in (("x", SPLIT[0]), ("y", SPLIT[1])):
        rows, token = permuted(at, count, pay)
        pay = summed(pay, axis, token)
        turned.append(rows)
        at += count
    turned.append(permuted(at, SPLIT[2], pay)[0])
    yt = call(
        turn_kernel, [((E, ROWS), BF16)], traits,
        grid_spec=pl.GridSpec(
            grid=(4,),
            in_specs=[pl.BlockSpec((ROWS, 256), lambda i: (0, i))],
            out_specs=pl.BlockSpec((256, ROWS), lambda i: (i, 0)),
        ),
        flops=10**9,
        room=6,
    )
    coef = call(solve_kernel, [((40, V + HALF), F32)], pay, shift(pay, "zh", 1), room=4, flops=10**8)
    far = shift(coef[:, V:], "core", 1)
    g1, g2, ss_v = call(
        geno_kernel,
        [((ROWS, CHUNK), BF16), ((ROWS, CHUNK), BF16), ((8, 128), F32)],
        coef, dx, *turned,
        flops=2 * 128 * ROWS * 2 * CHUNK,
        room=16,
    )
    rt, ss = call(
        resid_kernel,
        [((E, ROWS), BF16), ((SQUARES, 128), F32)],
        core, coef, far, yt, xt, ss_v,
        grid_spec=scalar_spec(5, 2),
        flops=2 * 128 * ROWS * E,
        room=12,
    )

    rt5 = rt.reshape(4, 2, 4, 32, ROWS)
    g_spec = pl.BlockSpec((ROWS, CHUNK), lambda i, t: (0, 0))
    ss_spec = pl.BlockSpec((SQUARES, 128), lambda i, t: (0, 0))

    def cross(axis, k, after):
        onx = axis == "x"
        low = LANES * 128 + (SQUARES if onx else 0)
        return call(
            cross1_kernel if onx else cross2_kernel,
            [((low, 128), F32), ((LANES * 128, 128), F32)],
            ((x if onx else y) + k) % 4,
            *((rt5, g1, ss) if onx else (rt, g2)),
            after,
            grid_spec=pltpu.PrefetchScalarGridSpec(
                num_scalar_prefetch=1,
                grid=(1,),
                in_specs=[
                    *(
                        (pl.BlockSpec((4, 2, 1, 32, ROWS), lambda i, t: (0, 0, t[0], 0, 0)), g_spec, ss_spec)
                        if onx
                        else (pl.BlockSpec((256, ROWS), lambda i, t: (t[0], 0)), g_spec)
                    ),
                    anywhere,
                ],
                out_specs=[
                    pl.BlockSpec((low, 128), lambda i, t: (0, 0)),
                    pl.BlockSpec((LANES * 128, 128), lambda i, t: (0, 0)),
                ],
            ),
            flops=2 * 256 * ROWS * CHUNK,
            room=10,
        )

    part, got = {}, {}
    after = ss
    for k in (2, 3, 1, 0):
        for axis in ("x", "y"):
            part[axis, k] = cross(axis, k, after)
            after = part[axis, k][1]
            low, high = part[axis, k]
            if k == 2:
                got[axis, "low2"] = shift(low, axis, 1)
                got[axis, "high2"] = shift(high, axis, 3)
            elif k == 1:
                got[axis, "high"] = shift(high, axis, 1)
            elif k == 3:
                got[axis, "low"] = shift(low, axis, 3)
    parts = {}
    whole = pl.BlockSpec(memory_space=pltpu.VMEM)
    for axis in ("x", "y"):
        relayed = []
        for k, half, name in ((1, 0, "low2"), (3, 1, "high2")):
            mine = part[axis, k][half]
            relayed.append(
                call(
                    relay_kernel, [(mine.shape, F32)], mine, got[axis, name], after,
                    in_specs=[whole, whole, anywhere], room=2,
                )
            )
        got[axis, "lows"] = shift(relayed[0], axis, 1)
        got[axis, "highs"] = shift(relayed[1], axis, 3)
    keeps = []
    for axis, other, at in (("x", "y", y), ("y", "x", x)):
        rows = LANES * 64 + (SQUARES if axis == "x" else 0)
        low, high = part[axis, 0]
        parts[axis] = call(
            mid_kernel, [((rows, 128), F32)] * 4, at,
            low, got[axis, "low"], got[axis, "lows"], high, got[axis, "high"], got[axis, "highs"],
            grid_spec=scalar_spec(6, 4), flops=10**7, room=4,
        )
        for k in (1, 2, 3):
            parts[axis][k] = shift(parts[axis][k], other, k)
    for axis in ("x", "y"):
        rows = LANES * 32 + (SQUARES if axis == "x" else 0)
        keep, send = call(
            last_kernel, [((rows, 128), F32)] * 2, zh, *parts[axis],
            grid_spec=scalar_spec(4, 2), flops=10**6, room=2,
        )
        keeps.append((keep, shift(send, "zh", 1)))
    observed, peaks, scales = call(
        score1_kernel, [((32, V), F32), ((32, 128), F32), ((40, 128), F32)], samp, *keeps[0],
        grid_spec=scalar_spec(2, 3), flops=10**6, room=4,
    )
    peaks = call(score2_kernel, [((8, 128), F32)], *keeps[1], peaks, scales, flops=10**6, room=4)
    peaks = jnp.maximum(peaks, shift(peaks, "core", 1))
    perm_max = call(
        peak_kernel, [((PERMS, 32), F32)], peaks, *(shift(peaks, "zl", k) for k in (1, 2, 3)),
        room=2,
    )
    return observed, perm_max


def solution(mesh):
    fine = Mesh(mesh.devices.reshape(4, 2, 4, 4, 2), ("y", "zh", "x", "zl", "core"))
    samp, tile = ("y", "zh", "x"), ("zl", "core")
    return jax.shard_map(
        program,
        mesh=fine,
        in_specs=(P(samp, None), P(samp, None), P(samp, tile), P(None, samp)),
        out_specs=(P(samp, tile), P(None, samp)),
        check_vma=False,
    )
```
